512 devices in a mesh: seq: 64 (over z, x), img: 8 (over y, core).
Axes of the slice: x: 4, y: 4, z: 16, core: 2. Of those that a mesh axis runs over, the one named last changes fastest.
Arguments:
- inner_acts: bfloat16 [65536, 3072], P(('img', 'seq')), parts along dimension 0, may hold values from -6 to 6
- gate_acts: bfloat16 [65536, 3072], P(('img', 'seq')), parts along dimension 0, may hold values from -6 to 6
- state_proj: bfloat16 [65536, 64], P(('img', 'seq')), parts along dimension 0, may hold values from -3 to 3
- step_raw: bfloat16 [65536, 96], P(('img', 'seq')), parts along dimension 0, may hold values from -4 to 4
- conv_weight: float32 [2, 4, 3072], replicated, may hold values from -3 to 3
- conv_bias: float32 [2, 3072], replicated, may hold values from -3 to 3
- step_bias: float32 [2, 48], replicated, may hold values from -1.5 to 0.5
- decay_rate: float32 [2, 48], replicated, may hold values from 5e-06 to 0.04
- skip_gain: float32 [2, 48], replicated, may hold values from 0.5 to 2
- norm_gain: float32 [3072], replicated, may hold values from 0.5 to 1.5
Outputs:
- mixed: bfloat16 [65536, 3072], P(('img', 'seq')), parts along dimension 0
The draws below stay inside these ranges and needn't reach their ends.
There are 8 independent parts, one for each index of `img`. The reference program is written for one: setup_inputs(seed, part) draws one part's arguments, and reference() takes and returns one part's arrays. A program takes and returns all parts, laid end to end along the dimension named above; an argument that names none is the same for every part. Nothing has to cross between parts.
All inputs are finite; a program needn't handle non-finite values.
Results may differ from the reference program's by a relative error of at most 0.0058.
Values may be sent and summed in bfloat16 or wider, within the bound.
A program may use at most 192 MiB of HBM per device.

```python
import math
import jax
import jax.numpy as jnp
from jax import lax

INNER = 3072
STATE = 16
KERNEL = 4
TOK_DEV = 128
HEADS = 48
TOKENS = 8192


def draw_step_raw(key, part):
    blocks = TOKENS // TOK_DEV
    offset_key = jax.random.fold_in(key, 11)
    noise_key = jax.random.fold_in(key, 12)
    offset = jax.random.uniform(offset_key, (blocks, 1, 2 * HEADS), jnp.float32, -3.0, 3.0)
    noise = jax.random.normal(noise_key, (blocks, TOK_DEV, 2 * HEADS), jnp.float32)
    values = jnp.clip(offset + noise, -4.0, 4.0)
    return values.reshape(TOKENS, 2 * HEADS).astype(jnp.bfloat16)


def shard_levels(rng, shape, split, low, high):
    level = 1.0
    for position, parts in split:
        draws = jax.random.uniform(jax.random.fold_in(jax.random.fold_in(rng, 6), position), (parts,), jnp.float32, low / len(split), high / len(split))
        level = level * jnp.repeat(jnp.exp(draws), shape[position] // parts).reshape((-1,) + (1,) * (len(shape) - 1 - position))
    return level


def gaussian(key, dims, deviation, limit, cuts=(), held_as=jnp.bfloat16):
    loudness = shard_levels(key, dims, cuts, -0.22, 0.18) if cuts else 1.0
    drawn = jax.random.normal(key, dims, jnp.float32) * deviation * loudness
    return jnp.minimum(jnp.maximum(drawn, -limit), limit).astype(held_as)


def setup_inputs(seed: int = 0, part: int = 0) -> dict:
    key_of = jax.random.split(jax.random.key(seed), 11)
    own_keys = jax.random.split(jax.random.fold_in(key_of[10], part), 11)
    return {
        "inner_acts": gaussian(own_keys[0], (TOKENS, INNER), 1.0, 6.0, ((0, 64),)),
        "gate_acts": gaussian(own_keys[1], (TOKENS, INNER), 1.0, 6.0, ((0, 64),)),
        "state_proj": gaussian(own_keys[2], (TOKENS, 4 * STATE), 0.5, 3.0, ((0, 64),)),
        "step_raw": draw_step_raw(jax.random.fold_in(jax.random.fold_in(key_of[10], part), 71), part),
        "conv_weight": gaussian(key_of[4], (2, KERNEL, INNER), 0.5, 3.0, (), jnp.float32),
        "conv_bias": gaussian(key_of[5], (2, INNER), 0.5, 3.0, (), jnp.float32),
        "step_bias": jnp.clip(jax.random.uniform(key_of[6], (2, HEADS), jnp.float32, -1.5, 0.5), -1.5, 0.5),
        "decay_rate": jnp.clip(jnp.exp(jax.random.uniform(key_of[7], (2, HEADS), jnp.float32, math.log(4.999999873689376e-06), math.log(0.04))), 4.999999873689376e-06, 0.04),
        "skip_gain": jnp.clip(jnp.exp(jax.random.uniform(key_of[8], (2, HEADS), jnp.float32, math.log(0.5), math.log(2.0))), 0.5, 2.0),
        "norm_gain": jnp.clip(1.0 + 0.1 * jax.random.normal(key_of[9], (INNER,), jnp.float32), 0.5, 1.5),
    }


def convolve(window, weight, bias):
    kernel = weight.shape[0]
    length = window.shape[0] - kernel + 1
    accum = jnp.zeros((length, window.shape[1]), jnp.float32) + bias[None, :]
    for offset in range(kernel):
        start = kernel - 1 - offset
        accum = accum + weight[offset][None, :] * window[start:start + length].astype(jnp.float32)
    return jax.nn.silu(accum).astype(jnp.bfloat16)

def block_terms(conved, write_rows, read_rows, raw_step, step_bias, rate, skip):
    length, width = conved.shape
    heads = raw_step.shape[1]
    step_size = jax.nn.softplus(raw_step.astype(jnp.float32) + step_bias[None, :])
    cumul = jnp.cumsum(-rate[None, :] * step_size, axis=0)
    later = lax.broadcasted_iota(jnp.int32, (length, length), 0)
    earlier = lax.broadcasted_iota(jnp.int32, (length, length), 1)
    causal = (later >= earlier)[None]
    spread = cumul.T[:, :, None] - cumul.T[:, None, :]
    decay = jnp.where(causal, jnp.exp(jnp.where(causal, spread, 0.0)), 0.0)
    scores = jnp.dot(read_rows, write_rows.T, preferred_element_type=jnp.float32)
    weights = (scores[None] * decay * step_size.T[:, None, :]).astype(jnp.bfloat16)
    per_head = conved.reshape(length, heads, width // heads)
    inside = jnp.einsum('hts,shp->thp', weights.astype(jnp.float32), per_head.astype(jnp.float32))
    final_log = cumul[-1]
    carried = jnp.exp(final_log[None, :] - cumul) * step_size
    loaded = (carried[:, :, None] * write_rows.astype(jnp.float32)[:, None, :]).astype(jnp.bfloat16)
    end_state = jnp.einsum('shp,shn->hpn', per_head.astype(jnp.float32), loaded.astype(jnp.float32))
    base = inside + skip[None, :, None] * per_head.astype(jnp.float32)
    return (base, cumul, jnp.exp(final_log), end_state)

def inter_terms(cumul, read_rows, incoming):
    readout = jnp.einsum('tn,hpn->thp', read_rows.astype(jnp.float32), incoming, precision=lax.Precision.HIGHEST)
    return readout * jnp.exp(cumul)[:, :, None]

def direction(acts, write_rows, read_rows, raw_step, weight, bias, step_bias, rate, skip):
    kernel = weight.shape[0]
    width = acts.shape[1]
    heads = raw_step.shape[1]
    window = jnp.concatenate([jnp.zeros((kernel - 1, width), acts.dtype), acts], axis=0)
    conved = convolve(window, weight, bias)
    blocks = conved.shape[0] // TOK_DEV
    pieces = (conved.reshape(blocks, TOK_DEV, width), write_rows.reshape(blocks, TOK_DEV, -1), read_rows.reshape(blocks, TOK_DEV, -1), raw_step.reshape(blocks, TOK_DEV, heads))

    def advance(incoming, piece):
        conved_block, write_block, read_block, raw_block = piece
        base, cumul, total, end_state = block_terms(conved_block, write_block, read_block, raw_block, step_bias, rate, skip)
        result = (base + inter_terms(cumul, read_block, incoming)).reshape(TOK_DEV, width)
        return (total[:, None, None] * incoming + end_state, result)
    initial = jnp.zeros((heads, width // heads, write_rows.shape[1]), jnp.float32)
    final_state, outputs = lax.scan(advance, initial, pieces)
    return outputs.reshape(-1, width)

def reference(inner_acts, gate_acts, state_proj, step_raw, conv_weight, conv_bias, step_bias, decay_rate, skip_gain, norm_gain):
    forward = direction(inner_acts, state_proj[:, 0:STATE], state_proj[:, STATE:2 * STATE], step_raw[:, :HEADS], conv_weight[0], conv_bias[0], step_bias[0], decay_rate[0], skip_gain[0])
    flipped_proj = state_proj[::-1]
    backward = direction(inner_acts[::-1], flipped_proj[:, 2 * STATE:3 * STATE], flipped_proj[:, 3 * STATE:4 * STATE], step_raw[::-1][:, HEADS:], conv_weight[1], conv_bias[1], step_bias[1], decay_rate[1], skip_gain[1])[::-1]
    gated = (forward + backward) * jax.nn.silu(gate_acts.astype(jnp.float32))
    scale = lax.rsqrt(lax.optimization_barrier(jnp.mean(gated * gated, axis=1, keepdims=True)) + 1e-05)
    return (gated * scale * norm_gain[None, :]).astype(jnp.bfloat16)
```

```python
import functools

import jax
import jax.numpy as jnp
from jax import lax
from jax.experimental import pallas as pl
from jax.experimental.pallas import tpu as pltpu
from jax.sharding import PartitionSpec as P

MESH = pl.DeviceIdType.MESH
F32 = jnp.float32
BF16 = jnp.bfloat16
LANES = 128
HEAD = 64
GROUP = 8


def split(v):
    high = v.astype(BF16).astype(F32)
    return jnp.concatenate([high, v - high], axis=1).astype(BF16)


def spreader(block, heads, rows):
    row = lax.broadcasted_iota(jnp.int32, (rows, LANES), 0)
    lane = lax.broadcasted_iota(jnp.int32, (rows, LANES), 1)
    row = jnp.where(row >= heads, row - heads, row)
    head = 2 * block + jnp.where(lane >= HEAD, 1, 0)
    return jnp.where(row == head, 1.0, 0.0).astype(BF16)


def dot(a, b):
    return jnp.dot(a, b, preferred_element_type=F32)


def silu(v):
    half = 0.5 * v
    return half + half * jnp.tanh(half)


def kernel(
    n, group, heads, kernel_taps,
    x_hbm, gate_hbm, proj_hbm, raw_hbm, cw_hbm, cb_hbm, sb_hbm, rate_hbm, skip_hbm, gain_hbm,
    out_hbm,
    xb, gb, ob, xs, cf, cr, gf, gr, u, ef, er,
    proj_v, raw_v, cw_v, cb_v, sb_v, rate_v, skip_v, gain_v,
    lhs_g, lhs_e, lhs_x, mf, mr, bt, cm,
    prev_v, next_v, tot_v, tots_v, totg_v, totr_v,
    send1, recv1, send2, recv2, send3, recv3, sumsq,
    x_sem, g_sem, o_sem, s_sem, h_send, h_recv,
    t1_send, t1_recv, t2_send, t2_recv, c1_send, c1_recv, c2_send, c2_recv, c3_send, c3_recv,
):
    rows = xb.shape[1]
    blocks = xb.shape[0]
    per = blocks // group
    groups = n // group
    states = bt.shape[1]
    me = lax.axis_index("seq")
    mem = lax.rem(me, group)
    grp = lax.div(me, group)
    base = me - mem

    def lanes(j):
        return pl.ds(pl.multiple_of(j * LANES, LANES), LANES)

    def member(r):
        return lax.rem(mem + r, group)

    def far(r):
        return lax.rem(grp + r, groups)

    small = [
        (raw_hbm, raw_v), (sb_hbm, sb_v), (rate_hbm, rate_v), (proj_hbm, proj_v),
        (skip_hbm, skip_v), (cw_hbm, cw_v), (cb_hbm, cb_v), (gain_hbm, gain_v),
    ]
    loads = [pltpu.make_async_copy(a, b, s_sem.at[i]) for i, (a, b) in enumerate(small)]
    for copy in loads:
        copy.start()

    def x_copy(j):
        return pltpu.make_async_copy(x_hbm.at[:, lanes(j)], xb.at[j], x_sem.at[j])

    def g_copy(j):
        return pltpu.make_async_copy(gate_hbm.at[:, lanes(j)], gb.at[j], g_sem.at[j])

    def o_copy(j):
        return pltpu.make_async_copy(ob.at[j], out_hbm.at[:, lanes(j)], o_sem.at[j])

    def start_x(j, carry):
        x_copy(j).start()
        return carry

    lax.fori_loop(0, blocks, start_x, 0)

    barrier = pltpu.get_barrier_semaphore()
    after = lax.rem(me + 1, n)
    before = lax.rem(me + n - 1, n)
    for peer in (after, before):
        pl.semaphore_signal(barrier, inc=1, device_id={"seq": peer}, device_id_type=MESH)

    def greet_group(r, carry):
        pl.semaphore_signal(
            barrier, inc=1, device_id={"seq": base + member(r)}, device_id_type=MESH
        )
        return carry

    def greet_far(r, carry):
        pl.semaphore_signal(
            barrier, inc=1, device_id={"seq": far(r) * group + mem}, device_id_type=MESH
        )
        return carry

    lax.fori_loop(1, groups, greet_far, 0)
    lax.fori_loop(1, group, greet_group, 0)

    def start_g(j, carry):
        g_copy(j).start()
        return carry

    lax.fori_loop(0, blocks, start_g, 0)
    for copy in loads:
        copy.wait()

    later = lax.broadcasted_iota(jnp.int32, (rows, rows), 0)
    earlier = lax.broadcasted_iota(jnp.int32, (rows, rows), 1)
    masks = (later >= earlier, later <= earlier)
    lasts = (rows - 1, 0)
    raw = raw_v[...].astype(F32)
    proj = proj_v[...].astype(F32)
    proj_t = proj.T
    zeros = jnp.zeros((16 - 2, heads), F32)
    grow, decay, total, skips = [], [], [], []
    for d in range(2):
        v = raw[:, d * heads : (d + 1) * heads] + sb_v[d : d + 1, :]
        step = jnp.maximum(v, 0.0) + jnp.log1p(jnp.exp(-jnp.abs(v)))
        tri = jnp.where(masks[d], 1.0, 0.0)
        cumul = jnp.dot(
            tri, -rate_v[d : d + 1, :] * step, precision=lax.Precision.HIGHEST,
            preferred_element_type=F32,
        )
        grow.append(jnp.exp(-cumul) * step)
        decay.append(jnp.exp(cumul))
        total.append(jnp.exp(cumul[lasts[d] : lasts[d] + 1, :]))
        skips.append(skip_v[d : d + 1, :])
        first = 2 * d * states
        write_t = proj_t[first : first + states, :].astype(BF16)
        read = proj[:, first + states : first + 2 * states].astype(BF16)
        bt[d] = write_t
        cm[d] = read
        scores = jnp.where(masks[d], dot(read, write_t), 0.0).astype(BF16)
        (mf, mr)[d][...] = scores
    lhs_g[...] = split(jnp.concatenate(grow, axis=0))
    lhs_e[...] = split(jnp.concatenate(decay + skips + [zeros], axis=0))
    lhs_x[...] = split(
        jnp.concatenate([grow[0][:16], grow[1][rows - 16 :]] + total + [zeros], axis=0)
    )
    tot_v[...] = jnp.concatenate(
        [
            jnp.concatenate(total + [jnp.zeros((6, heads), F32)], axis=0),
            jnp.zeros((8, LANES - heads), F32),
        ],
        axis=1,
    )

    def taps(d, j, first, count):
        acc = jnp.zeros((count, LANES), F32) + cb_v[d : d + 1, lanes(j)]
        for k in range(kernel_taps):
            shift = -k if d == 0 else k
            acc = acc + cw_v[d, k : k + 1, lanes(j)] * xs[j, pl.ds(8 + first + shift, count), :]
        return silu(acc).astype(BF16)

    def conv(j, carry):
        x_copy(j).wait()
        xs[j, pl.ds(0, 8), :] = jnp.zeros((8, LANES), F32)
        xs[j, pl.ds(8 + rows, 8), :] = jnp.zeros((8, LANES), F32)
        xs[j, pl.ds(8, rows), :] = xb[j].astype(F32)
        wide = dot(lhs_g[...], spreader(j, heads, 2 * heads))
        for d in range(2):
            conved = taps(d, j, 0, rows)
            (cf, cr)[d][j] = conved
            scaled = wide[d * rows : (d + 1) * rows] * conved.astype(F32)
            (gf, gr)[d][j] = scaled.astype(BF16)
        return carry

    lax.fori_loop(0, blocks, conv, 0)

    pl.semaphore_wait(barrier, 2 + (groups - 1) + (group - 1))
    edge = 8
    halo = [
        pltpu.make_async_remote_copy(
            src_ref=x_hbm.at[pl.ds(rows - edge, edge)], dst_ref=prev_v,
            send_sem=h_send.at[0], recv_sem=h_recv.at[0],
            device_id={"seq": after}, device_id_type=MESH,
        ),
        pltpu.make_async_remote_copy(
            src_ref=x_hbm.at[pl.ds(0, edge)], dst_ref=next_v,
            send_sem=h_send.at[1], recv_sem=h_recv.at[1],
            device_id={"seq": before}, device_id_type=MESH,
        ),
    ]
    for copy in halo:
        copy.start()

    def near_copy(src, dst, ss, rs, r):
        return pltpu.make_async_remote_copy(
            src_ref=src, dst_ref=dst, send_sem=ss.at[r - 1], recv_sem=rs.at[r - 1],
            device_id={"seq": base + member(r)}, device_id_type=MESH,
        )

    def far_copy(src, dst, ss, rs, r):
        return pltpu.make_async_remote_copy(
            src_ref=src, dst_ref=dst, send_sem=ss.at[r - 1], recv_sem=rs.at[r - 1],
            device_id={"seq": far(r) * group + mem}, device_id_type=MESH,
        )

    def t1(r):
        return near_copy(tot_v, tots_v.at[mem], t1_send, t1_recv, r)

    def t2(r):
        return far_copy(totg_v, totr_v.at[grp], t2_send, t2_recv, r)

    def c1(r):
        return near_copy(send1.at[member(r)], recv1.at[mem], c1_send, c1_recv, r)

    def c2(r):
        ahead = jnp.where(far(r) > grp, 0, 1)
        return far_copy(send2.at[ahead], recv2.at[grp], c2_send, c2_recv, r)

    def c3(r):
        return near_copy(send3.at[member(r)], recv3.at[mem], c3_send, c3_recv, r)

    def loop(first, last, action):
        def body(r, carry):
            action(r)
            return carry

        lax.fori_loop(first, last, body, 0)

    loop(1, group, lambda r: t1(r).start())
    tots_v[mem] = tot_v[...]

    for copy in halo:
        copy.wait()
    loop(1, group, lambda r: t1(r).wait())

    def edges(j, carry):
        has_before = jnp.where(me > 0, 1.0, 0.0)
        has_after = jnp.where(me < n - 1, 1.0, 0.0)
        xs[j, pl.ds(0, 8), :] = prev_v[:, lanes(j)].astype(F32) * has_before
        xs[j, pl.ds(8 + rows, 8), :] = next_v[:, lanes(j)].astype(F32) * has_after
        return carry

    lax.fori_loop(0, blocks, edges, 0)

    def finish(j, place, buffer):
        wide = dot(lhs_x[...], spreader(j, heads, 2 * heads))
        ends = []
        for d in range(2):
            first = (0, rows - 16)[d]
            conved = taps(d, j, first, 16)
            (cf, cr)[d][j, pl.ds(first, 16), :] = conved
            scaled = wide[d * 16 : (d + 1) * 16] * conved.astype(F32)
            (gf, gr)[d][j, pl.ds(first, 16), :] = scaled.astype(BF16)
            end = dot(bt[d], (gf, gr)[d][j]) * wide[32 + d : 33 + d]
            ends.append(end)
        buffer[place] = jnp.concatenate(ends, axis=0).astype(BF16)

    def ends(r):
        owner = member(r)
        for b in range(per):
            finish(owner * per + b, (owner, b), send1)
        c1(r).start()

    loop(1, group, ends)
    for b in range(per):
        finish(mem * per + b, (mem, b), recv1)

    product = tots_v[0]
    for m in range(1, group):
        product = product * tots_v[m]
    totg_v[...] = product
    loop(1, groups, lambda r: t2(r).start())
    totr_v[grp] = product

    def inner(j, carry):
        g_copy(j).wait()
        wide = dot(lhs_e[...], spreader(j, heads, 2 * heads))
        gate = silu(gb[j].astype(F32))
        far_f, far_r = wide[:rows] * gate, wide[rows : 2 * rows] * gate
        ef[j] = far_f
        er[j] = far_r
        direct = (
            wide[2 * rows : 2 * rows + 1] * cf[j].astype(F32)
            + wide[2 * rows + 1 : 2 * rows + 2] * cr[j].astype(F32)
        )
        u[j] = (
            direct * gate + far_f * dot(mf[...], gf[j]) + far_r * dot(mr[...], gr[j])
        )
        return carry

    lax.fori_loop(0, blocks, inner, 0)

    loop(1, group, lambda r: c1(r).wait_recv())

    def spread(values, b):
        flat = values[...].reshape(-1, LANES)
        high = flat.astype(BF16)
        low = (flat - high.astype(F32)).astype(BF16)
        ones = spreader(mem * per + b, LANES, LANES)
        return dot(high, ones) + dot(low, ones)

    near_t = [spread(tots_v, b) for b in range(per)]

    def part(ref, m, b, d):
        return ref[m, b, pl.ds(d * states, states), :].astype(F32)

    for b in range(per):
        run_f = jnp.zeros((states, LANES), F32)
        run_r = jnp.zeros((states, LANES), F32)
        for m in range(group):
            run_f = run_f * near_t[b][8 * m : 8 * m + 1] + part(recv1, m, b, 0)
            k = group - 1 - m
            run_r = run_r * near_t[b][8 * k + 1 : 8 * k + 2] + part(recv1, k, b, 1)
        send2[0, b] = run_f.astype(BF16)
        send2[1, b] = run_r.astype(BF16)
    loop(1, groups, lambda r: c2(r).start())
    loop(1, groups, lambda r: t2(r).wait())
    far_t = [spread(totr_v, b) for b in range(per)]
    recv2[grp] = send2[0]
    loop(1, groups, lambda r: c2(r).wait_recv())

    for b in range(per):
        run_f = jnp.zeros((states, LANES), F32)
        run_r = jnp.zeros((states, LANES), F32)
        for g in range(groups):
            new = run_f * far_t[b][8 * g : 8 * g + 1] + recv2[g, b].astype(F32)
            run_f = jnp.where(g < grp, new, run_f)
            k = groups - 1 - g
            new = run_r * far_t[b][8 * k + 1 : 8 * k + 2] + recv2[k, b].astype(F32)
            run_r = jnp.where(k > grp, new, run_r)
        for m in range(group):
            send3[m, b, pl.ds(0, states), :] = run_f.astype(BF16)
            run_f = run_f * near_t[b][8 * m : 8 * m + 1] + part(recv1, m, b, 0)
            k = group - 1 - m
            send3[k, b, pl.ds(states, states), :] = run_r.astype(BF16)
            run_r = run_r * near_t[b][8 * k + 1 : 8 * k + 2] + part(recv1, k, b, 1)
    loop(1, group, lambda r: c3(r).start())
    recv3[mem] = send3[mem]

    sumsq[...] = jnp.zeros_like(sumsq)

    def outer(owner):
        for b in range(per):
            j = owner * per + b
            gated = (
                u[j]
                + ef[j] * dot(cm[0], recv3[owner, b, pl.ds(0, states), :])
                + er[j] * dot(cm[1], recv3[owner, b, pl.ds(states, states), :])
            )
            u[j] = gated
            sumsq[...] += gated * gated

    outer(mem)

    def arrived(r):
        c3(r).wait_recv()
        outer(lax.rem(mem + group - r, group))

    loop(1, group, arrived)
    mean = jnp.sum(sumsq[...], axis=1, keepdims=True) * (1.0 / (blocks * LANES))
    scale = lax.rsqrt(mean + 1e-05)

    def write(j, carry):
        ob[j] = (u[j] * scale * gain_v[:, lanes(j)]).astype(BF16)
        o_copy(j).start()
        return carry

    lax.fori_loop(0, blocks, write, 0)
    loop(1, group, lambda r: c1(r).wait_send())
    loop(1, groups, lambda r: c2(r).wait_send())
    loop(1, group, lambda r: c3(r).wait_send())
    loop(0, blocks, lambda j: o_copy(j).wait())


def solution(mesh, group=GROUP, interpret=False):
    n = mesh.shape["seq"]

    def local(inner, gate, proj, raw, conv_weight, conv_bias, step_bias, rate, skip, gain):
        rows, width = inner.shape
        heads = width // HEAD
        blocks = width // LANES
        per = blocks // group
        groups = n // group
        states = proj.shape[1] // 4
        taps = conv_weight.shape[1]
        dma = pltpu.SemaphoreType.DMA
        vm = pltpu.VMEM
        scratch = [
            vm((blocks, rows, LANES), BF16),
            vm((blocks, rows, LANES), BF16),
            vm((blocks, rows, LANES), BF16),
            vm((blocks, rows + 16, LANES), F32),
            vm((blocks, rows, LANES), BF16),
            vm((blocks, rows, LANES), BF16),
            vm((blocks, rows, LANES), BF16),
            vm((blocks, rows, LANES), BF16),
            vm((blocks, rows, LANES), F32),
            vm((blocks, rows, LANES), F32),
            vm((blocks, rows, LANES), F32),
            vm(proj.shape, BF16),
            vm(raw.shape, BF16),
            vm(conv_weight.shape, F32),
            vm(conv_bias.shape, F32),
            vm(step_bias.shape, F32),
            vm(rate.shape, F32),
            vm(skip.shape, F32),
            vm((1, width), F32),
            vm((2 * rows, 2 * heads), BF16),
            vm((2 * rows + 16, 2 * heads), BF16),
            vm((48, 2 * heads), BF16),
            vm((rows, rows), BF16),
            vm((rows, rows), BF16),
            vm((2, states, rows), BF16),
            vm((2, rows, states), BF16),
            vm((8, width), BF16),
            vm((8, width), BF16),
            vm((8, LANES), F32),
            vm((group, 8, LANES), F32),
            vm((8, LANES), F32),
            vm((groups, 8, LANES), F32),
            vm((group, per, 2 * states, LANES), BF16),
            vm((group, per, 2 * states, LANES), BF16),
            vm((2, per, states, LANES), BF16),
            vm((groups, per, states, LANES), BF16),
            vm((group, per, 2 * states, LANES), BF16),
            vm((group, per, 2 * states, LANES), BF16),
            vm((rows, LANES), F32),
            dma((blocks,)),
            dma((blocks,)),
            dma((blocks,)),
            dma((8,)),
            dma((2,)),
            dma((2,)),
        ]
        near, far = dma((group - 1,)), dma((groups - 1,))
        scratch += [near, near, far, far, near, near, far, far, near, near]
        return pl.pallas_call(
            functools.partial(kernel, n, group, heads, taps),
            out_shape=jax.ShapeDtypeStruct((rows, width), BF16),
            in_specs=[pl.BlockSpec(memory_space=pl.ANY)] * 10,
            out_specs=pl.BlockSpec(memory_space=pl.ANY),
            scratch_shapes=scratch,
            compiler_params=pltpu.CompilerParams(
                collective_id=0, has_side_effects=True, vmem_limit_bytes=56 * 2**20
            ),
            name="mixer",
            interpret=interpret,
        )(
            inner, gate, proj, raw, conv_weight, conv_bias, step_bias, rate, skip,
            gain.reshape(1, width),
        )

    spec = P(("img", "seq"), None)
    return jax.shard_map(
        local,
        mesh=mesh,
        in_specs=(spec, spec, spec, spec, P(), P(), P(), P(), P(), P()),
        out_specs=spec,
        check_vma=False,
    )
```

```python
import functools

import jax
import jax.numpy as jnp
from jax import lax
from jax.experimental import pallas as pl
from jax.experimental.pallas import tpu as pltpu
from jax.sharding import PartitionSpec as P

MESH = pl.DeviceIdType.MESH
F32 = jnp.float32
BF16 = jnp.bfloat16
LANES = 128
HEAD = 64
GROUP = 8


def split(v):
    high = v.astype(BF16).astype(F32)
    return jnp.concatenate([high, v - high], axis=1).astype(BF16)


def spreader(block, heads, rows):
    row = lax.broadcasted_iota(jnp.int32, (rows, LANES), 0)
    lane = lax.broadcasted_iota(jnp.int32, (rows, LANES), 1)
    row = jnp.where(row >= heads, row - heads, row)
    head = 2 * block + jnp.where(lane >= HEAD, 1, 0)
    return jnp.where(row == head, 1.0, 0.0).astype(BF16)


def dot(a, b):
    return jnp.dot(a, b, preferred_element_type=F32)


def silu(v):
    half = 0.5 * v
    return half + half * jnp.tanh(half)


def kernel(
    n, group, heads, kernel_taps,
    x_hbm, gate_hbm, proj_hbm, raw_hbm, cw_hbm, cb_hbm, sb_hbm, rate_hbm, skip_hbm,
    u, sumsq,
    xb, gb, xs, cf, cr, gf, gr, sg, ef, er, end0, gx, ext,
    proj_v, raw_v, cw_v, cb_v, sb_v, rate_v, skip_v,
    lhs_g, lhs_e, mf, mr, btm, bte, cm,
    prev_v, next_v, tot_v, tots_v, totg_v, totr_v,
    send1, recv1, send2, recv2, send3, recv3,
    x_sem, g_sem, s_sem, h_send, h_recv,
    t1_send, t1_recv, t2_send, t2_recv, c1_send, c1_recv, c2_send, c2_recv, c3_send, c3_recv,
):
    rows = xb.shape[1]
    blocks = xb.shape[0]
    per = blocks // group
    groups = n // group
    states = btm.shape[1]
    me = lax.axis_index("seq")
    mem = lax.rem(me, group)
    grp = lax.div(me, group)
    base = me - mem

    def lanes(j):
        return pl.ds(pl.multiple_of(j * LANES, LANES), LANES)

    def member(r):
        return lax.rem(mem + r, group)

    def far(r):
        return lax.rem(grp + r, groups)

    small = [
        (raw_hbm, raw_v), (sb_hbm, sb_v), (rate_hbm, rate_v), (proj_hbm, proj_v),
        (skip_hbm, skip_v), (cw_hbm, cw_v), (cb_hbm, cb_v),
    ]
    loads = [pltpu.make_async_copy(a, b, s_sem.at[i]) for i, (a, b) in enumerate(small)]
    for copy in loads:
        copy.start()

    def x_copy(j):
        return pltpu.make_async_copy(x_hbm.at[:, lanes(j)], xb.at[j], x_sem.at[j])

    def g_copy(j):
        return pltpu.make_async_copy(gate_hbm.at[:, lanes(j)], gb.at[j], g_sem.at[j])

    def start_x(j, carry):
        x_copy(j).start()
        return carry

    lax.fori_loop(0, blocks, start_x, 0)

    barrier = pltpu.get_barrier_semaphore()
    after = lax.rem(me + 1, n)
    before = lax.rem(me + n - 1, n)
    for peer in (after, before):
        pl.semaphore_signal(barrier, inc=1, device_id={"seq": peer}, device_id_type=MESH)

    def greet_group(r, carry):
        pl.semaphore_signal(
            barrier, inc=1, device_id={"seq": base + member(r)}, device_id_type=MESH
        )
        return carry

    def greet_far(r, carry):
        pl.semaphore_signal(
            barrier, inc=1, device_id={"seq": far(r) * group + mem}, device_id_type=MESH
        )
        return carry

    lax.fori_loop(1, groups, greet_far, 0)
    lax.fori_loop(1, group, greet_group, 0)

    def start_g(j, carry):
        g_copy(j).start()
        return carry

    lax.fori_loop(0, blocks, start_g, 0)
    for copy in loads:
        copy.wait()

    first_t = lax.broadcasted_iota(jnp.int32, (rows, rows), 0)
    second_t = lax.broadcasted_iota(jnp.int32, (rows, rows), 1)
    masks = (first_t >= second_t, first_t <= second_t)
    lasts = (rows - 1, 0)
    column = lax.broadcasted_iota(jnp.int32, (states, rows), 1)
    edge_rows = (column < 16, column >= rows - 16)
    raw = raw_v[...].astype(F32)
    params = jnp.concatenate(
        [
            jnp.concatenate([sb_v[...], rate_v[...], jnp.zeros((4, heads), F32)], axis=0),
            jnp.zeros((8, LANES - heads), F32),
        ],
        axis=1,
    ).T
    zeros = jnp.zeros((16 - 4, heads), F32)
    grow, decay, total, skips = [], [], [], []
    for d in range(2):
        v = raw[d * heads : (d + 1) * heads] + params[:heads, d : d + 1]
        step = jnp.maximum(v, 0.0) + jnp.log1p(jnp.exp(-jnp.abs(v)))
        cumul = jnp.dot(
            -params[:heads, 2 + d : 3 + d] * step,
            jnp.where(masks[1 - d], 1.0, 0.0),
            precision=lax.Precision.HIGHEST,
            preferred_element_type=F32,
        )
        grow.append((jnp.exp(-cumul) * step).T)
        decay.append(jnp.exp(cumul).T)
        total.append(decay[d][lasts[d] : lasts[d] + 1, :])
        skips.append(skip_v[d : d + 1, :])
        first = 2 * d * states
        write_t = proj_v[first : first + states, :]
        read = proj_v[first + states : first + 2 * states, :].astype(F32).T.astype(BF16)
        btm[d] = jnp.where(edge_rows[d], 0.0, write_t.astype(F32)).astype(BF16)
        bte[d] = (write_t[:, :16], write_t[:, rows - 16 :])[d]
        cm[d] = read
        scores = jnp.where(masks[d], dot(read, write_t), 0.0).astype(BF16)
        (mf, mr)[d][...] = scores
    lhs_g[...] = split(jnp.concatenate(grow + total + skips + [zeros], axis=0))
    lhs_e[...] = split(jnp.concatenate(decay, axis=0))
    tot_v[...] = jnp.concatenate(
        [
            jnp.concatenate(total + [jnp.zeros((6, heads), F32)], axis=0),
            jnp.zeros((8, LANES - heads), F32),
        ],
        axis=1,
    )

    def taps(d, j, first, count):
        acc = jnp.zeros((count, LANES), F32) + cb_v[d : d + 1, lanes(j)]
        for k in range(kernel_taps):
            shift = -k if d == 0 else k
            acc = acc + cw_v[d, k : k + 1, lanes(j)] * xs[j, pl.ds(8 + first + shift, count), :]
        return silu(acc).astype(BF16)

    def conv(j, carry):
        x_copy(j).wait()
        xs[j, pl.ds(0, 8), :] = jnp.zeros((8, LANES), F32)
        xs[j, pl.ds(8 + rows, 8), :] = jnp.zeros((8, LANES), F32)
        xs[j, pl.ds(8, rows), :] = xb[j].astype(F32)
        wide = dot(lhs_g[...], spreader(j, heads, 2 * heads))
        gx[j, pl.ds(0, 16), :] = wide[:16]
        gx[j, pl.ds(16, 16), :] = wide[2 * rows - 16 : 2 * rows]
        ext[j] = wide[2 * rows : 2 * rows + 8]
        for d in range(2):
            conved = taps(d, j, 0, rows)
            (cf, cr)[d][j] = conved
            scaled = (wide[d * rows : (d + 1) * rows] * conved.astype(F32)).astype(BF16)
            (gf, gr)[d][j] = scaled
            end0[j, pl.ds(d * states, states), :] = dot(btm[d], scaled)
        return carry

    lax.fori_loop(0, blocks, conv, 0)

    pl.semaphore_wait(barrier, 2 + (groups - 1) + (group - 1))
    edge = 8
    halo = [
        pltpu.make_async_remote_copy(
            src_ref=xb.at[:, pl.ds(rows - edge, edge), :], dst_ref=prev_v,
            send_sem=h_send.at[0], recv_sem=h_recv.at[0],
            device_id={"seq": after}, device_id_type=MESH,
        ),
        pltpu.make_async_remote_copy(
            src_ref=xb.at[:, pl.ds(0, edge), :], dst_ref=next_v,
            send_sem=h_send.at[1], recv_sem=h_recv.at[1],
            device_id={"seq": before}, device_id_type=MESH,
        ),
    ]
    for copy in halo:
        copy.start()

    def near_copy(src, dst, ss, rs, r):
        return pltpu.make_async_remote_copy(
            src_ref=src, dst_ref=dst, send_sem=ss.at[r - 1], recv_sem=rs.at[r - 1],
            device_id={"seq": base + member(r)}, device_id_type=MESH,
        )

    def far_copy(src, dst, ss, rs, r):
        return pltpu.make_async_remote_copy(
            src_ref=src, dst_ref=dst, send_sem=ss.at[r - 1], recv_sem=rs.at[r - 1],
            device_id={"seq": far(r) * group + mem}, device_id_type=MESH,
        )

    def t1(r):
        return near_copy(tot_v, tots_v.at[mem], t1_send, t1_recv, r)

    def t2(r):
        return far_copy(totg_v, totr_v.at[grp], t2_send, t2_recv, r)

    def c1(r):
        return near_copy(send1.at[member(r)], recv1.at[mem], c1_send, c1_recv, r)

    def c2(r):
        ahead = jnp.where(far(r) > grp, 0, 1)
        return far_copy(send2.at[ahead], recv2.at[grp], c2_send, c2_recv, r)

    def c3(r):
        return near_copy(send3.at[member(r)], recv3.at[mem], c3_send, c3_recv, r)

    def loop(first, last, action):
        def body(r, carry):
            action(r)
            return carry

        lax.fori_loop(first, last, body, 0)

    loop(1, group, lambda r: t1(r).start())
    tots_v[mem] = tot_v[...]

    def outside(j, carry):
        g_copy(j).wait()
        wide = dot(lhs_e[...], spreader(j, heads, 2 * heads))
        gate = silu(gb[j].astype(F32))
        sg[j] = gate
        ef[j] = wide[:rows] * gate
        er[j] = wide[rows:] * gate
        return carry

    lax.fori_loop(0, blocks, outside, 0)

    loop(1, group, lambda r: t1(r).wait())
    product = tots_v[0]
    for m in range(1, group):
        product = product * tots_v[m]
    totg_v[...] = product
    loop(1, groups, lambda r: t2(r).start())
    totr_v[grp] = product

    for copy in halo:
        copy.wait()

    def edges(j, carry):
        has_before = jnp.where(me > 0, 1.0, 0.0)
        has_after = jnp.where(me < n - 1, 1.0, 0.0)
        xs[j, pl.ds(0, 8), :] = prev_v[j].astype(F32) * has_before
        xs[j, pl.ds(8 + rows, 8), :] = next_v[j].astype(F32) * has_after
        return carry

    lax.fori_loop(0, blocks, edges, 0)

    def finish(owner, buffer):
        results = []
        for b in range(per):
            j = owner * per + b
            for d in range(2):
                first = (0, rows - 16)[d]
                conved = taps(d, j, first, 16)
                scaled = (gx[j, pl.ds(16 * d, 16), :] * conved.astype(F32)).astype(BF16)
                end = end0[j, pl.ds(d * states, states), :] + dot(bte[d], scaled)
                end = (end * ext[j, pl.ds(d, 1), :]).astype(BF16)
                results.append((b, j, d, first, conved, scaled, end))
        for b, j, d, first, conved, scaled, end in results:
            (cf, cr)[d][j, pl.ds(first, 16), :] = conved
            (gf, gr)[d][j, pl.ds(first, 16), :] = scaled
            buffer[owner, b, pl.ds(d * states, states), :] = end

    def ends(r):
        owner = member(r)
        finish(owner, send1)
        c1(r).start()

    loop(1, group, ends)
    finish(mem, recv1)

    def inner(j, carry):
        direct = (
            ext[j, pl.ds(2, 1), :] * cf[j].astype(F32) + ext[j, pl.ds(3, 1), :] * cr[j].astype(F32)
        )
        u[j] = (
            direct * sg[j] + ef[j] * dot(mf[...], gf[j]) + er[j] * dot(mr[...], gr[j])
        )
        return carry

    lax.fori_loop(0, blocks, inner, 0)

    loop(1, group, lambda r: c1(r).wait_recv())

    def spread(values, b):
        flat = values[...].reshape(-1, LANES)
        high = flat.astype(BF16)
        low = (flat - high.astype(F32)).astype(BF16)
        ones = spreader(mem * per + b, LANES, LANES)
        return dot(high, ones) + dot(low, ones)

    near_t = [spread(tots_v, b) for b in range(per)]

    def part(ref, m, b, d):
        return ref[m, b, pl.ds(d * states, states), :].astype(F32)

    for b in range(per):
        run_f = jnp.zeros((states, LANES), F32)
        run_r = jnp.zeros((states, LANES), F32)
        for m in range(group):
            run_f = run_f * near_t[b][8 * m : 8 * m + 1] + part(recv1, m, b, 0)
            k = group - 1 - m
            run_r = run_r * near_t[b][8 * k + 1 : 8 * k + 2] + part(recv1, k, b, 1)
        send2[0, b] = run_f.astype(BF16)
        send2[1, b] = run_r.astype(BF16)
    loop(1, groups, lambda r: c2(r).start())
    loop(1, groups, lambda r: t2(r).wait())
    far_t = [spread(totr_v, b) for b in range(per)]
    recv2[grp] = send2[0]
    loop(1, groups, lambda r: c2(r).wait_recv())

    for b in range(per):
        run_f = jnp.zeros((states, LANES), F32)
        run_r = jnp.zeros((states, LANES), F32)
        for g in range(groups):
            new = run_f * far_t[b][8 * g : 8 * g + 1] + recv2[g, b].astype(F32)
            run_f = jnp.where(g < grp, new, run_f)
            k = groups - 1 - g
            new = run_r * far_t[b][8 * k + 1 : 8 * k + 2] + recv2[k, b].astype(F32)
            run_r = jnp.where(k > grp, new, run_r)
        for m in range(group):
            send3[m, b, pl.ds(0, states), :] = run_f.astype(BF16)
            run_f = run_f * near_t[b][8 * m : 8 * m + 1] + part(recv1, m, b, 0)
            k = group - 1 - m
            send3[k, b, pl.ds(states, states), :] = run_r.astype(BF16)
            run_r = run_r * near_t[b][8 * k + 1 : 8 * k + 2] + part(recv1, k, b, 1)
    loop(1, group, lambda r: c3(r).start())
    recv3[mem] = send3[mem]

    sumsq[...] = jnp.zeros_like(sumsq)

    def outer(owner):
        for b in range(per):
            j = owner * per + b
            gated = (
                u[j]
                + ef[j] * dot(cm[0], recv3[owner, b, pl.ds(0, states), :])
                + er[j] * dot(cm[1], recv3[owner, b, pl.ds(states, states), :])
            )
            u[j] = gated
            sumsq[...] += gated * gated

    outer(mem)

    def arrived(r):
        c3(r).wait_recv()
        outer(lax.rem(mem + group - r, group))

    loop(1, group, arrived)
    loop(1, group, lambda r: c1(r).wait_send())
    loop(1, groups, lambda r: c2(r).wait_send())
    loop(1, group, lambda r: c3(r).wait_send())


def finale(u, sumsq, gain_hbm, out_hbm, ob, gain_v, o_sem, s_sem):
    blocks = ob.shape[0]
    load = pltpu.make_async_copy(gain_hbm, gain_v, s_sem)
    load.start()
    mean = jnp.sum(sumsq[...], axis=1, keepdims=True) * (1.0 / (blocks * LANES))
    scale = lax.rsqrt(mean + 1e-05)
    load.wait()

    def o_copy(j):
        return pltpu.make_async_copy(ob.at[j], out_hbm.at[:, pl.ds(j * LANES, LANES)], o_sem.at[j])

    for j in range(blocks):
        ob[j] = (u[j] * scale * gain_v[:, pl.ds(j * LANES, LANES)]).astype(BF16)
        o_copy(j).start()
    for j in range(blocks):
        o_copy(j).wait()


def solution(mesh, group=GROUP):
    n = mesh.shape["seq"]

    def local(inner, gate, proj, raw, conv_weight, conv_bias, step_bias, rate, skip, gain):
        rows, width = inner.shape
        heads = width // HEAD
        blocks = width // LANES
        per = blocks // group
        groups = n // group
        states = proj.shape[1] // 4
        taps = conv_weight.shape[1]
        dma = pltpu.SemaphoreType.DMA
        vm = pltpu.VMEM
        wide16 = vm((blocks, rows, LANES), BF16)
        wide32 = vm((blocks, rows, LANES), F32)
        scratch = [
            wide16,
            wide16,
            vm((blocks, rows + 16, LANES), F32),
            wide16,
            wide16,
            wide16,
            wide16,
            wide32,
            wide32,
            wide32,
            vm((blocks, 2 * states, LANES), F32),
            vm((blocks, 32, LANES), F32),
            vm((blocks, 8, LANES), F32),
            vm(proj.shape[::-1], BF16),
            vm(raw.shape[::-1], BF16),
            vm(conv_weight.shape, F32),
            vm(conv_bias.shape, F32),
            vm(step_bias.shape, F32),
            vm(rate.shape, F32),
            vm(skip.shape, F32),
            vm((2 * rows + 16, 2 * heads), BF16),
            vm((2 * rows, 2 * heads), BF16),
            vm((rows, rows), BF16),
            vm((rows, rows), BF16),
            vm((2, states, rows), BF16),
            vm((2, states, 16), BF16),
            vm((2, rows, states), BF16),
            vm((blocks, 8, LANES), BF16),
            vm((blocks, 8, LANES), BF16),
            vm((8, LANES), F32),
            vm((group, 8, LANES), F32),
            vm((8, LANES), F32),
            vm((groups, 8, LANES), F32),
            vm((group, per, 2 * states, LANES), BF16),
            vm((group, per, 2 * states, LANES), BF16),
            vm((2, per, states, LANES), BF16),
            vm((groups, per, states, LANES), BF16),
            vm((group, per, 2 * states, LANES), BF16),
            vm((group, per, 2 * states, LANES), BF16),
            dma((blocks,)),
            dma((blocks,)),
            dma((8,)),
            dma((2,)),
            dma((2,)),
        ]
        near, far = dma((group - 1,)), dma((groups - 1,))
        scratch += [near, near, far, far, near, near, far, far, near, near]
        vmem = pl.BlockSpec(memory_space=pltpu.VMEM)
        hbm = pl.BlockSpec(memory_space=pl.ANY)
        gated, sumsq = pl.pallas_call(
            functools.partial(kernel, n, group, heads, taps),
            out_shape=(
                jax.ShapeDtypeStruct((blocks, rows, LANES), F32),
                jax.ShapeDtypeStruct((rows, LANES), F32),
            ),
            in_specs=[hbm] * 9,
            out_specs=(vmem, vmem),
            scratch_shapes=scratch,
            compiler_params=pltpu.CompilerParams(
                collective_id=0, has_side_effects=True, vmem_limit_bytes=36 * 2**20
            ),
            name="mixer",
        )(
            *(
                pltpu.with_memory_space_constraint(array, pltpu.HBM)
                for array in (
                    inner, gate, proj.T, raw.T, conv_weight, conv_bias, step_bias, rate, skip
                )
            )
        )
        return pl.pallas_call(
            finale,
            out_shape=jax.ShapeDtypeStruct((rows, width), BF16),
            in_specs=[vmem, vmem, hbm],
            out_specs=hbm,
            scratch_shapes=[wide16, vm((1, width), F32), dma((blocks,)), dma],
            compiler_params=pltpu.CompilerParams(vmem_limit_bytes=16 * 2**20),
            name="finale",
        )(gated, sumsq, gain.reshape(1, width))

    spec = P(("img", "seq"), None)
    return jax.shard_map(
        local,
        mesh=mesh,
        in_specs=(spec, spec, spec, spec, P(), P(), P(), P(), P(), P()),
        out_specs=spec,
        check_vma=False,
    )
```

```python
import functools

import jax
import jax.numpy as jnp
from jax import lax
from jax.experimental import pallas as pl
from jax.experimental.pallas import tpu as pltpu
from jax.sharding import PartitionSpec as P

MESH = pl.DeviceIdType.MESH
F32 = jnp.float32
BF16 = jnp.bfloat16
LANES = 128
HEAD = 64
GROUP = 8
BAND = 32


def split(v):
    high = v.astype(BF16).astype(F32)
    return jnp.concatenate([high, v - high], axis=1).astype(BF16)


def spreader(block, heads, rows):
    row = lax.broadcasted_iota(jnp.int32, (rows, LANES), 0)
    lane = lax.broadcasted_iota(jnp.int32, (rows, LANES), 1)
    row = jnp.where(row >= heads, row - heads, row)
    head = 2 * block + jnp.where(lane >= HEAD, 1, 0)
    return jnp.where(row == head, 1.0, 0.0).astype(BF16)


def dot(a, b):
    return jnp.dot(a, b, preferred_element_type=F32)


def silu(v):
    half = 0.5 * v
    return half + half * jnp.tanh(half)


def kernel(
    n, group, heads, kernel_taps,
    x_hbm, gate_hbm, proj_hbm, raw_hbm, cw_hbm, cb_hbm, sb_hbm, rate_hbm, skip_hbm,
    u, sumsq,
    xb, gb, xs, cf, cr, gf, gr, sg, ef, er, gw, ext,
    proj_v, raw_v, cw_v, cb_v, sb_v, rate_v, skip_v,
    lhs, mf, mr, bt, cm,
    prev_v, next_v, tot_v, tots_v, totg_v, totr_v,
    send1, recv1, send2, recv2, send3, recv3,
    x_sem, g_sem, s_sem, ready, h_send, h_recv,
    t1_send, t1_recv, t2_send, t2_recv, c1_send, c1_recv, c2_send, c2_recv, c3_send, c3_recv,
):
    rows = u.shape[1]
    blocks = u.shape[0]
    per = blocks // group
    groups = n // group
    states = bt.shape[1]
    me = lax.axis_index("seq")
    mem = lax.rem(me, group)
    grp = lax.div(me, group)
    base = me - mem

    def lanes(j):
        return pl.ds(pl.multiple_of(j * LANES, LANES), LANES)

    def member(r):
        return lax.rem(mem + r, group)

    def far(r):
        return lax.rem(grp + r, groups)

    def sweep(body, many):
        def turn(i, carry):
            for q in range(many):
                body(i * many + q)
            return carry

        lax.fori_loop(0, blocks // many, turn, 0)

    small = [
        (raw_hbm, raw_v), (sb_hbm, sb_v), (rate_hbm, rate_v), (proj_hbm, proj_v),
        (skip_hbm, skip_v), (cw_hbm, cw_v), (cb_hbm, cb_v),
    ]
    loads = [pltpu.make_async_copy(a, b, s_sem.at[i]) for i, (a, b) in enumerate(small)]
    for copy in loads:
        copy.start()

    bands = rows // BAND

    def x_copy(i):
        band = pl.ds(i * BAND, BAND)
        return pltpu.make_async_copy(x_hbm.at[band], xb.at[band], x_sem.at[i])

    def g_copy(i):
        band = pl.ds(i * BAND, BAND)
        return pltpu.make_async_copy(gate_hbm.at[band], gb.at[band], g_sem.at[i])

    for i in range(bands):
        x_copy(i).start()

    barrier = pltpu.get_barrier_semaphore()
    after = lax.rem(me + 1, n)
    before = lax.rem(me + n - 1, n)
    beside = (lax.rem(me + group, n), lax.rem(me + n - group, n))

    def signal(semaphore, peer):
        pl.semaphore_signal(semaphore, inc=1, device_id={"seq": peer}, device_id_type=MESH)

    for peer in (after, before) + beside:
        signal(barrier, peer)
    for r in range(1, group):
        signal(barrier, base + member(r))

    for i in range(bands):
        g_copy(i).start()
    for copy in loads:
        copy.wait()

    first_t = lax.broadcasted_iota(jnp.int32, (rows, rows), 0)
    second_t = lax.broadcasted_iota(jnp.int32, (rows, rows), 1)
    masks = (first_t >= second_t, first_t <= second_t)
    lasts = (rows - 1, 0)
    raw = raw_v[...].astype(F32)
    params = jnp.concatenate(
        [
            jnp.concatenate([sb_v[...], rate_v[...], jnp.zeros((4, heads), F32)], axis=0),
            jnp.zeros((8, LANES - heads), F32),
        ],
        axis=1,
    ).T
    zeros = jnp.zeros((16 - 4, heads), F32)
    grow, decay, total, skips = [], [], [], []
    for d in range(2):
        v = raw[d * heads : (d + 1) * heads] + params[:heads, d : d + 1]
        step = jnp.maximum(v, 0.0) + jnp.log1p(jnp.exp(-jnp.abs(v)))
        cumul = jnp.dot(
            -params[:heads, 2 + d : 3 + d] * step,
            jnp.where(masks[1 - d], 1.0, 0.0),
            precision=lax.Precision.HIGHEST,
            preferred_element_type=F32,
        )
        grow.append((jnp.exp(-cumul) * step).T)
        decay.append(jnp.exp(cumul).T)
        total.append(decay[d][lasts[d] : lasts[d] + 1, :])
        skips.append(skip_v[d : d + 1, :])
        first = 2 * d * states
        write_t = proj_v[first : first + states, :]
        read = proj_v[first + states : first + 2 * states, :].astype(F32).T.astype(BF16)
        bt[d] = write_t
        cm[d] = read
        scores = jnp.where(masks[d], dot(read, write_t), 0.0).astype(BF16)
        (mf, mr)[d][...] = scores
    lhs[...] = split(jnp.concatenate(decay + grow + total + skips + [zeros], axis=0))
    tot_v[...] = jnp.concatenate(
        [
            jnp.concatenate(total + [jnp.zeros((6, heads), F32)], axis=0),
            jnp.zeros((8, LANES - heads), F32),
        ],
        axis=1,
    )

    for i in range(bands):
        x_copy(i).wait()
    pl.semaphore_wait(barrier, 4 + (group - 1))
    rounds = groups // 2 - 1

    def relay(k):
        if 0 < k <= rounds:
            pl.semaphore_wait(ready.at[k - 1], 2)
        if k < rounds:
            for peer in beside:
                signal(ready.at[k], peer)

    relay(0)
    edge = 8
    halo = [
        pltpu.make_async_remote_copy(
            src_ref=xb.at[pl.ds(rows - edge, edge)], dst_ref=prev_v,
            send_sem=h_send.at[0], recv_sem=h_recv.at[0],
            device_id={"seq": after}, device_id_type=MESH,
        ),
        pltpu.make_async_remote_copy(
            src_ref=xb.at[pl.ds(0, edge)], dst_ref=next_v,
            send_sem=h_send.at[1], recv_sem=h_recv.at[1],
            device_id={"seq": before}, device_id_type=MESH,
        ),
    ]
    for copy in halo:
        copy.start()

    def near_copy(src, dst, ss, rs, r):
        return pltpu.make_async_remote_copy(
            src_ref=src, dst_ref=dst, send_sem=ss.at[r - 1], recv_sem=rs.at[r - 1],
            device_id={"seq": base + member(r)}, device_id_type=MESH,
        )

    def far_copy(src, dst, ss, rs, r):
        return pltpu.make_async_remote_copy(
            src_ref=src, dst_ref=dst, send_sem=ss.at[r - 1], recv_sem=rs.at[r - 1],
            device_id={"seq": far(r) * group + mem}, device_id_type=MESH,
        )

    def t1(r):
        return near_copy(tot_v, tots_v.at[mem], t1_send, t1_recv, r)

    def t2(r):
        return far_copy(totg_v, totr_v.at[grp], t2_send, t2_recv, r)

    def c1(r):
        return near_copy(send1.at[member(r)], recv1.at[mem], c1_send, c1_recv, r)

    def c2(r):
        ahead = jnp.where(far(r) > grp, 0, 1)
        return far_copy(send2.at[ahead], recv2.at[grp], c2_send, c2_recv, r)

    def c3(r):
        return near_copy(send3.at[member(r)], recv3.at[mem], c3_send, c3_recv, r)

    def loop(first, last, action):
        def body(r, carry):
            action(r)
            return carry

        lax.fori_loop(first, last, body, 0)

    loop(1, group, lambda r: t1(r).start())
    tots_v[mem] = tot_v[...]

    for i in range(bands):
        g_copy(i).wait()

    def outside(j):
        wide = dot(lhs[...], spreader(j, heads, 2 * heads))
        gate = silu(gb[:, lanes(j)].astype(F32))
        sg[j] = gate
        ef[j] = wide[:rows] * gate
        er[j] = wide[rows : 2 * rows] * gate
        gw[0, j] = wide[2 * rows : 3 * rows]
        gw[1, j] = wide[3 * rows : 4 * rows]
        ext[j] = wide[4 * rows : 4 * rows + 8]

    sweep(outside, 3)
    for copy in halo:
        copy.wait()

    has_before = jnp.where(me > 0, 1.0, 0.0)
    has_after = jnp.where(me < n - 1, 1.0, 0.0)

    def conv(owner):
        for b in range(per):
            j = owner * per + b
            xs[j, pl.ds(0, 8), :] = prev_v[:, lanes(j)].astype(F32) * has_before
            xs[j, pl.ds(8 + rows, 8), :] = next_v[:, lanes(j)].astype(F32) * has_after
            xs[j, pl.ds(8, rows), :] = xb[:, lanes(j)].astype(F32)
        for b in range(per):
            j = owner * per + b
            for d in range(2):
                acc = 0.5 * cb_v[d : d + 1, lanes(j)]
                for k in range(kernel_taps):
                    shift = -k if d == 0 else k
                    tap = 0.5 * cw_v[d, k : k + 1, lanes(j)]
                    acc = acc + tap * xs[j, pl.ds(8 + shift, rows), :]
                conved = (acc + acc * jnp.tanh(acc)).astype(BF16)
                (cf, cr)[d][j] = conved
                (gf, gr)[d][j] = (gw[d, j] * conved.astype(F32)).astype(BF16)

    def finish(owner, buffer):
        results = []
        for b in range(per):
            j = owner * per + b
            for d in range(2):
                end = dot(bt[d], (gf, gr)[d][j]) * ext[j, pl.ds(d, 1), :]
                results.append((b, d, end.astype(BF16)))
        for b, d, end in results:
            buffer[owner, b, pl.ds(d * states, states), :] = end

    conv(member(1))

    def ends(r):
        finish(member(r), send1)
        conv(member(r + 1))
        c1(r).start()

    loop(1, group, ends)
    finish(mem, recv1)
    relay(1)

    loop(1, group, lambda r: t1(r).wait())
    product = tots_v[0]
    for m in range(1, group):
        product = product * tots_v[m]
    totg_v[...] = product
    totr_v[grp] = product

    def inner(j):
        direct = (
            ext[j, pl.ds(2, 1), :] * cf[j].astype(F32) + ext[j, pl.ds(3, 1), :] * cr[j].astype(F32)
        )
        u[j] = (
            direct * sg[j] + ef[j] * dot(mf[...], gf[j]) + er[j] * dot(mr[...], gr[j])
        )

    sweep(inner, 4)
    relay(2)

    loop(1, group, lambda r: c1(r).wait_recv())

    def spread(values, b):
        flat = values[...].reshape(-1, LANES)
        high = flat.astype(BF16)
        low = (flat - high.astype(F32)).astype(BF16)
        ones = spreader(mem * per + b, LANES, LANES)
        return dot(high, ones) + dot(low, ones)

    near_t = [spread(tots_v, b) for b in range(per)]

    def part(ref, m, b, d):
        return ref[m, b, pl.ds(d * states, states), :].astype(F32)

    for b in range(per):
        run_f = jnp.zeros((states, LANES), F32)
        run_r = jnp.zeros((states, LANES), F32)
        for m in range(group):
            run_f = run_f * near_t[b][8 * m : 8 * m + 1] + part(recv1, m, b, 0)
            k = group - 1 - m
            run_r = run_r * near_t[b][8 * k + 1 : 8 * k + 2] + part(recv1, k, b, 1)
        send2[0, b] = run_f.astype(BF16)
        send2[1, b] = run_r.astype(BF16)
    relay(3)
    loop(1, groups, lambda r: t2(r).start())
    loop(1, groups, lambda r: c2(r).start())
    loop(1, groups, lambda r: t2(r).wait())
    far_t = [spread(totr_v, b) for b in range(per)]
    recv2[grp] = send2[0]
    loop(1, groups, lambda r: c2(r).wait_recv())

    for b in range(per):
        run_f = jnp.zeros((states, LANES), F32)
        run_r = jnp.zeros((states, LANES), F32)
        for g in range(groups):
            new = run_f * far_t[b][8 * g : 8 * g + 1] + recv2[g, b].astype(F32)
            run_f = jnp.where(g < grp, new, run_f)
            k = groups - 1 - g
            new = run_r * far_t[b][8 * k + 1 : 8 * k + 2] + recv2[k, b].astype(F32)
            run_r = jnp.where(k > grp, new, run_r)
        for m in range(group):
            send3[m, b, pl.ds(0, states), :] = run_f.astype(BF16)
            run_f = run_f * near_t[b][8 * m : 8 * m + 1] + part(recv1, m, b, 0)
            k = group - 1 - m
            send3[k, b, pl.ds(states, states), :] = run_r.astype(BF16)
            run_r = run_r * near_t[b][8 * k + 1 : 8 * k + 2] + part(recv1, k, b, 1)
    loop(1, group, lambda r: c3(r).start())
    recv3[mem] = send3[mem]

    sumsq[...] = jnp.zeros_like(sumsq)

    def outer(owner):
        for b in range(per):
            j = owner * per + b
            gated = (
                u[j]
                + ef[j] * dot(cm[0], recv3[owner, b, pl.ds(0, states), :])
                + er[j] * dot(cm[1], recv3[owner, b, pl.ds(states, states), :])
            )
            u[j] = gated
            sumsq[...] += gated * gated

    outer(mem)

    def arrived(r):
        c3(r).wait_recv()
        outer(lax.rem(mem + group - r, group))

    loop(1, group, arrived)
    loop(1, group, lambda r: c1(r).wait_send())
    loop(1, groups, lambda r: c2(r).wait_send())
    loop(1, group, lambda r: c3(r).wait_send())


def finale(u, sumsq, gain_hbm, out_hbm, ob, gain_v, o_sem, s_sem):
    blocks, rows, _ = u.shape
    load = pltpu.make_async_copy(gain_hbm, gain_v, s_sem)
    load.start()
    mean = jnp.sum(sumsq[...], axis=1, keepdims=True) * (1.0 / (blocks * LANES))
    scale = lax.rsqrt(mean + 1e-05)
    load.wait()

    def o_copy(i):
        band = pl.ds(i * BAND, BAND)
        return pltpu.make_async_copy(ob.at[band], out_hbm.at[band], o_sem.at[i])

    for i in range(rows // BAND):
        part = slice(i * BAND, (i + 1) * BAND)
        for j in range(blocks):
            lanes = slice(j * LANES, (j + 1) * LANES)
            ob[part, lanes] = (u[j, part] * scale[part] * gain_v[:, lanes]).astype(BF16)
        o_copy(i).start()
    for i in range(rows // BAND):
        o_copy(i).wait()


def solution(mesh, group=GROUP):
    n = mesh.shape["seq"]

    def local(inner, gate, proj, raw, conv_weight, conv_bias, step_bias, rate, skip, gain):
        rows, width = inner.shape
        heads = width // HEAD
        blocks = width // LANES
        per = blocks // group
        groups = n // group
        states = proj.shape[1] // 4
        taps = conv_weight.shape[1]
        dma = pltpu.SemaphoreType.DMA
        vm = pltpu.VMEM
        wide16 = vm((blocks, rows, LANES), BF16)
        wide32 = vm((blocks, rows, LANES), F32)
        scratch = [
            vm((rows, width), BF16),
            vm((rows, width), BF16),
            vm((blocks, rows + 16, LANES), F32),
            wide16,
            wide16,
            wide16,
            wide16,
            wide32,
            wide32,
            wide32,
            vm((2, blocks, rows, LANES), F32),
            vm((blocks, 8, LANES), F32),
            vm(proj.shape[::-1], BF16),
            vm(raw.shape[::-1], BF16),
            vm(conv_weight.shape, F32),
            vm(conv_bias.shape, F32),
            vm(step_bias.shape, F32),
            vm(rate.shape, F32),
            vm(skip.shape, F32),
            vm((4 * rows + 16, 2 * heads), BF16),
            vm((rows, rows), BF16),
            vm((rows, rows), BF16),
            vm((2, states, rows), BF16),
            vm((2, rows, states), BF16),
            vm((8, width), BF16),
            vm((8, width), BF16),
            vm((8, LANES), F32),
            vm((group, 8, LANES), F32),
            vm((8, LANES), F32),
            vm((groups, 8, LANES), F32),
            vm((group, per, 2 * states, LANES), BF16),
            vm((group, per, 2 * states, LANES), BF16),
            vm((2, per, states, LANES), BF16),
            vm((groups, per, states, LANES), BF16),
            vm((group, per, 2 * states, LANES), BF16),
            vm((group, per, 2 * states, LANES), BF16),
            dma((rows // BAND,)),
            dma((rows // BAND,)),
            dma((8,)),
            pltpu.SemaphoreType.REGULAR((max(1, groups // 2 - 1),)),
            dma((2,)),
            dma((2,)),
        ]
        near, far = dma((group - 1,)), dma((groups - 1,))
        scratch += [near, near, far, far, near, near, far, far, near, near]
        vmem = pl.BlockSpec(memory_space=pltpu.VMEM)
        hbm = pl.BlockSpec(memory_space=pl.ANY)
        gated, sumsq = pl.pallas_call(
            functools.partial(kernel, n, group, heads, taps),
            out_shape=(
                jax.ShapeDtypeStruct((blocks, rows, LANES), F32),
                jax.ShapeDtypeStruct((rows, LANES), F32),
            ),
            in_specs=[hbm] * 9,
            out_specs=(vmem, vmem),
            scratch_shapes=scratch,
            compiler_params=pltpu.CompilerParams(
                collective_id=0, has_side_effects=True, vmem_limit_bytes=36 * 2**20
            ),
            name="mixer",
        )(
            *(
                pltpu.with_memory_space_constraint(array, pltpu.HBM)
                for array in (
                    inner, gate, proj.T, raw.T, conv_weight, conv_bias, step_bias, rate, skip
                )
            )
        )
        return pl.pallas_call(
            finale,
            out_shape=jax.ShapeDtypeStruct((rows, width), BF16),
            in_specs=[vmem, vmem, hbm],
            out_specs=hbm,
            scratch_shapes=[
                vm((rows, width), BF16), vm((1, width), F32), dma((rows // BAND,)), dma
            ],
            compiler_params=pltpu.CompilerParams(vmem_limit_bytes=16 * 2**20),
            name="finale",
        )(gated, sumsq, gain.reshape(1, width))

    spec = P(("img", "seq"), None)
    return jax.shard_map(
        local,
        mesh=mesh,
        in_specs=(spec, spec, spec, spec, P(), P(), P(), P(), P(), P()),
        out_specs=spec,
        check_vma=False,
    )
```

```python
import functools

import jax
import jax.numpy as jnp
from jax import lax
from jax.experimental import pallas as pl
from jax.experimental.pallas import tpu as pltpu
from jax.sharding import PartitionSpec as P

MESH = pl.DeviceIdType.MESH
F32 = jnp.float32
BF16 = jnp.bfloat16
LANES = 128
HEAD = 64
GROUP = 8
NEAR = (6, 5, 7, 2, 4, 1, 3)
FAR = (4, 3, 5, 2, 6, 1, 7)
BAND = 32


def split(v):
    high = v.astype(BF16).astype(F32)
    return jnp.concatenate([high, v - high], axis=1).astype(BF16)


def spreader(block, heads, rows):
    row = lax.broadcasted_iota(jnp.int32, (rows, LANES), 0)
    lane = lax.broadcasted_iota(jnp.int32, (rows, LANES), 1)
    row = jnp.where(row >= heads, row - heads, row)
    head = 2 * block + jnp.where(lane >= HEAD, 1, 0)
    return jnp.where(row == head, 1.0, 0.0).astype(BF16)


def dot(a, b):
    return jnp.dot(a, b, preferred_element_type=F32)


def silu(v):
    half = 0.5 * v
    return half + half * jnp.tanh(half)


def kernel(
    n, group, heads, kernel_taps,
    x_hbm, gate_hbm, proj_hbm, raw_hbm, cw_hbm, cb_hbm, sb_hbm, rate_hbm, skip_hbm,
    u, sumsq,
    xb, gb, xs, cf, cr, gf, gr, ef, er, gw, ext,
    proj_v, raw_v, cw_v, cb_v, sb_v, rate_v, skip_v,
    lhs, mf, mr, bt, cm,
    prev_v, next_v, tot_v, tots_v, totg_v, totr_v,
    send1, recv1, send2, recv2, send3, recv3,
    x_sem, g_sem, s_sem, ready, h_send, h_recv,
    t1_send, t1_recv, t2_send, t2_recv, c1_send, c1_recv, c2_send, c2_recv, c3_send, c3_recv,
):
    rows = u.shape[1]
    blocks = u.shape[0]
    per = blocks // group
    groups = n // group
    states = bt.shape[1]
    me = lax.axis_index("seq")
    mem = lax.rem(me, group)
    grp = lax.div(me, group)
    base = me - mem

    def lanes(j):
        return pl.ds(pl.multiple_of(j * LANES, LANES), LANES)

    def pick(table, r):
        found = 0
        for k, value in enumerate(table):
            found = found + jnp.where(r == k + 1, value, 0)
        return found

    def offset(r, way):
        if group != 8:
            return lax.rem(mem + way * r + group, group)
        code = pick(NEAR, r)
        across = lax.rem(lax.div(mem, 4) + lax.div(code, 4), 2)
        return across * 4 + lax.rem(lax.rem(mem, 4) + way * lax.rem(code, 4) + 4, 4)

    def member(r):
        return offset(r, 1)

    def far(r):
        return lax.rem(grp + (pick(FAR, r) if groups == 8 else r), groups)

    def sweep(body, many):
        def turn(i, carry):
            for q in range(many):
                body(i * many + q)
            return carry

        lax.fori_loop(0, blocks // many, turn, 0)

    small = [
        (raw_hbm, raw_v), (sb_hbm, sb_v), (rate_hbm, rate_v), (proj_hbm, proj_v),
        (skip_hbm, skip_v), (cw_hbm, cw_v), (cb_hbm, cb_v),
    ]
    loads = [pltpu.make_async_copy(a, b, s_sem.at[i]) for i, (a, b) in enumerate(small)]
    for copy in loads:
        copy.start()

    bands = rows // BAND

    def x_copy(i):
        band = pl.ds(i * BAND, BAND)
        return pltpu.make_async_copy(x_hbm.at[band], xb.at[band], x_sem)

    def g_copy(i):
        band = pl.ds(i * BAND, BAND)
        return pltpu.make_async_copy(gate_hbm.at[band], gb.at[band], g_sem)

    for i in range(bands):
        x_copy(i).start()

    barrier = pltpu.get_barrier_semaphore()
    after = lax.rem(me + 1, n)
    before = lax.rem(me + n - 1, n)
    beside = (lax.rem(me + group, n), lax.rem(me + n - group, n))

    def signal(semaphore, peer):
        pl.semaphore_signal(semaphore, inc=1, device_id={"seq": peer}, device_id_type=MESH)

    for peer in (after, before) + beside:
        signal(barrier, peer)
    for r in range(1, group):
        signal(barrier, base + member(r))

    for i in range(bands):
        g_copy(i).start()

    pl.semaphore_wait(barrier, 4 + (group - 1))
    edge = 8
    halo = [
        pltpu.make_async_remote_copy(
            src_ref=x_hbm.at[pl.ds(rows - edge, edge)], dst_ref=prev_v,
            send_sem=h_send.at[0], recv_sem=h_recv.at[0],
            device_id={"seq": after}, device_id_type=MESH,
        ),
        pltpu.make_async_remote_copy(
            src_ref=x_hbm.at[pl.ds(0, edge)], dst_ref=next_v,
            send_sem=h_send.at[1], recv_sem=h_recv.at[1],
            device_id={"seq": before}, device_id_type=MESH,
        ),
    ]
    for copy in halo:
        copy.start()
    rounds = groups // 2 - 1

    def relay(k):
        if 0 < k <= rounds:
            pl.semaphore_wait(ready.at[k - 1], 2)
        if k < rounds:
            for peer in beside:
                signal(ready.at[k], peer)

    relay(0)
    for copy in loads[:5]:
        copy.wait()

    first_t = lax.broadcasted_iota(jnp.int32, (rows, rows), 0)
    second_t = lax.broadcasted_iota(jnp.int32, (rows, rows), 1)
    masks = (first_t >= second_t, first_t <= second_t)
    lasts = (rows - 1, 0)
    raw = raw_v[...].astype(F32)
    params = jnp.concatenate(
        [
            jnp.concatenate([sb_v[...], rate_v[...], jnp.zeros((4, heads), F32)], axis=0),
            jnp.zeros((8, LANES - heads), F32),
        ],
        axis=1,
    ).T
    zeros = jnp.zeros((16 - 4, heads), F32)
    grow, decay, total, skips = [], [], [], []
    for d in range(2):
        v = raw[d * heads : (d + 1) * heads] + params[:heads, d : d + 1]
        step = jnp.maximum(v, 0.0) + jnp.log1p(jnp.exp(-jnp.abs(v)))
        cumul = jnp.dot(
            -params[:heads, 2 + d : 3 + d] * step,
            jnp.where(masks[1 - d], 1.0, 0.0),
            precision=lax.Precision.HIGHEST,
            preferred_element_type=F32,
        )
        grow.append((jnp.exp(-cumul) * step).T)
        decay.append(jnp.exp(cumul).T)
        total.append(decay[d][lasts[d] : lasts[d] + 1, :])
        skips.append(skip_v[d : d + 1, :])
        first = 2 * d * states
        write_t = proj_v[first : first + states, :]
        read = proj_v[first + states : first + 2 * states, :].astype(F32).T.astype(BF16)
        bt[d] = write_t
        cm[d] = read
        scores = jnp.where(masks[d], dot(read, write_t), 0.0).astype(BF16)
        (mf, mr)[d][...] = scores
    lhs[...] = split(jnp.concatenate(decay + grow + total + skips + [zeros], axis=0))
    tot_v[...] = jnp.concatenate(
        [
            jnp.concatenate(total + [jnp.zeros((6, heads), F32)], axis=0),
            jnp.zeros((8, LANES - heads), F32),
        ],
        axis=1,
    )

    def near_copy(src, dst, ss, rs, r):
        return pltpu.make_async_remote_copy(
            src_ref=src, dst_ref=dst, send_sem=ss, recv_sem=rs,
            device_id={"seq": base + member(r)}, device_id_type=MESH,
        )

    def far_copy(src, dst, ss, rs, r):
        return pltpu.make_async_remote_copy(
            src_ref=src, dst_ref=dst, send_sem=ss, recv_sem=rs,
            device_id={"seq": far(r) * group + mem}, device_id_type=MESH,
        )

    def t1(r):
        return near_copy(tot_v, tots_v.at[mem], t1_send, t1_recv, r)

    def t2(r):
        return far_copy(totg_v, totr_v.at[grp], t2_send, t2_recv, r)

    def c1(r):
        return near_copy(send1.at[member(r)], recv1.at[mem], c1_send, c1_recv, r)

    def c2(r):
        ahead = jnp.where(far(r) > grp, 0, 1)
        return far_copy(send2.at[ahead], recv2.at[grp], c2_send, c2_recv, r)

    def c3(r):
        return near_copy(send3.at[member(r)], recv3.at[mem], c3_send, c3_recv.at[r - 1], r)

    near_all, far_all = pl.ds(0, group - 1), pl.ds(0, groups - 1)
    t1_all = near_copy(tots_v.at[near_all], tots_v.at[near_all], t1_send, t1_recv, 1)
    t2_all = far_copy(totr_v.at[far_all], totr_v.at[far_all], t2_send, t2_recv, 1)
    c1_all = near_copy(send1.at[near_all], recv1.at[near_all], c1_send, c1_recv, 1)
    c2_all = far_copy(recv2.at[far_all], recv2.at[far_all], c2_send, c2_recv, 1)
    c3_all = near_copy(send3.at[near_all], recv3.at[near_all], c3_send, c3_recv.at[0], 1)

    def loop(first, last, action):
        def body(r, carry):
            action(r)
            return carry

        lax.fori_loop(first, last, body, 0)

    loop(1, group, lambda r: t1(r).start())
    tots_v[mem] = tot_v[...]

    def growth(j):
        wide = dot(lhs[pl.ds(2 * rows, 2 * rows + 16), :], spreader(j, heads, 2 * heads))
        gw[0, j] = wide[:rows]
        gw[1, j] = wide[rows : 2 * rows]
        ext[j] = wide[2 * rows : 2 * rows + 8]

    sweep(growth, 3)
    relay(1)
    for copy in loads[5:]:
        copy.wait()
    pltpu.make_async_copy(x_hbm, xb, x_sem).wait()
    for copy in halo:
        copy.wait()

    has_before = jnp.where(me > 0, 1.0, 0.0)
    has_after = jnp.where(me < n - 1, 1.0, 0.0)

    def conv(owner):
        for b in range(per):
            j = owner * per + b
            xs[j, pl.ds(0, 8), :] = prev_v[:, lanes(j)].astype(F32) * has_before
            xs[j, pl.ds(8 + rows, 8), :] = next_v[:, lanes(j)].astype(F32) * has_after
            xs[j, pl.ds(8, rows), :] = xb[:, lanes(j)].astype(F32)
        for b in range(per):
            j = owner * per + b
            for d in range(2):
                acc = 0.5 * cb_v[d : d + 1, lanes(j)]
                for k in range(kernel_taps):
                    shift = -k if d == 0 else k
                    tap = 0.5 * cw_v[d, k : k + 1, lanes(j)]
                    acc = acc + tap * xs[j, pl.ds(8 + shift, rows), :]
                conved = (acc + acc * jnp.tanh(acc)).astype(BF16)
                (cf, cr)[d][j] = conved
                (gf, gr)[d][j] = (gw[d, j] * conved.astype(F32)).astype(BF16)

    def finish(owner, buffer):
        results = []
        for b in range(per):
            j = owner * per + b
            for d in range(2):
                end = dot(bt[d], (gf, gr)[d][j]) * ext[j, pl.ds(d, 1), :]
                results.append((b, d, end.astype(BF16)))
        for b, d, end in results:
            buffer[owner, b, pl.ds(d * states, states), :] = end

    conv(member(1))

    def ends(r):
        finish(member(r), send1)
        conv(member(r + 1))
        c1(r).start()

    loop(1, group, ends)
    finish(mem, recv1)
    relay(2)

    t1_all.wait()
    product = tots_v[0]
    for m in range(1, group):
        product = product * tots_v[m]
    totg_v[...] = product
    totr_v[grp] = product
    pltpu.make_async_copy(gate_hbm, gb, g_sem).wait()

    def inner(j):
        wide = dot(lhs[pl.ds(0, 2 * rows), :], spreader(j, heads, 2 * heads))
        gate = silu(gb[:, lanes(j)].astype(F32))
        far_f, far_r = wide[:rows] * gate, wide[rows:] * gate
        ef[j] = far_f
        er[j] = far_r
        direct = (
            ext[j, pl.ds(2, 1), :] * cf[j].astype(F32) + ext[j, pl.ds(3, 1), :] * cr[j].astype(F32)
        )
        u[j] = direct * gate + far_f * dot(mf[...], gf[j]) + far_r * dot(mr[...], gr[j])

    sweep(inner, 3)
    relay(3)
    loop(1, groups, lambda r: t2(r).start())

    c1_all.wait_recv()

    def spread(values, b):
        flat = values[...].reshape(-1, LANES)
        high = flat.astype(BF16)
        low = (flat - high.astype(F32)).astype(BF16)
        ones = spreader(mem * per + b, LANES, LANES)
        return dot(high, ones) + dot(low, ones)

    near_t = [spread(tots_v, b) for b in range(per)]

    def part(ref, m, b, d):
        return ref[m, b, pl.ds(d * states, states), :].astype(F32)

    for b in range(per):
        run_f = jnp.zeros((states, LANES), F32)
        run_r = jnp.zeros((states, LANES), F32)
        for m in range(group):
            run_f = run_f * near_t[b][8 * m : 8 * m + 1] + part(recv1, m, b, 0)
            k = group - 1 - m
            run_r = run_r * near_t[b][8 * k + 1 : 8 * k + 2] + part(recv1, k, b, 1)
        send2[0, b] = run_f.astype(BF16)
        send2[1, b] = run_r.astype(BF16)
    loop(1, groups, lambda r: c2(r).start())
    t2_all.wait()
    far_t = [spread(totr_v, b) for b in range(per)]
    recv2[grp] = send2[0]
    c2_all.wait_recv()

    for b in range(per):
        run_f = jnp.zeros((states, LANES), F32)
        run_r = jnp.zeros((states, LANES), F32)
        for g in range(groups):
            new = run_f * far_t[b][8 * g : 8 * g + 1] + recv2[g, b].astype(F32)
            run_f = jnp.where(g < grp, new, run_f)
            k = groups - 1 - g
            new = run_r * far_t[b][8 * k + 1 : 8 * k + 2] + recv2[k, b].astype(F32)
            run_r = jnp.where(k > grp, new, run_r)
        for m in range(group):
            send3[m, b, pl.ds(0, states), :] = run_f.astype(BF16)
            run_f = run_f * near_t[b][8 * m : 8 * m + 1] + part(recv1, m, b, 0)
            k = group - 1 - m
            send3[k, b, pl.ds(states, states), :] = run_r.astype(BF16)
            run_r = run_r * near_t[b][8 * k + 1 : 8 * k + 2] + part(recv1, k, b, 1)
    loop(1, group, lambda r: c3(r).start())
    recv3[mem] = send3[mem]

    sumsq[...] = jnp.zeros_like(sumsq)

    def outer(owner):
        for b in range(per):
            j = owner * per + b
            gated = (
                u[j]
                + ef[j] * dot(cm[0], recv3[owner, b, pl.ds(0, states), :])
                + er[j] * dot(cm[1], recv3[owner, b, pl.ds(states, states), :])
            )
            u[j] = gated
            sumsq[...] += gated * gated

    outer(mem)

    def arrived(r):
        c3(r).wait_recv()
        outer(offset(r, -1))

    loop(1, group, arrived)
    c1_all.wait_send()
    c2_all.wait_send()
    c3_all.wait_send()


def finale(u, sumsq, gain_hbm, out_hbm, ob, gain_v, o_sem, s_sem):
    blocks, rows, _ = u.shape
    load = pltpu.make_async_copy(gain_hbm, gain_v, s_sem)
    load.start()
    mean = jnp.sum(sumsq[...], axis=1, keepdims=True) * (1.0 / (blocks * LANES))
    scale = lax.rsqrt(mean + 1e-05)
    load.wait()

    def o_copy(i):
        band = pl.ds(i * BAND, BAND)
        return pltpu.make_async_copy(ob.at[band], out_hbm.at[band], o_sem)

    for i in range(rows // BAND):
        part = slice(i * BAND, (i + 1) * BAND)
        for j in range(blocks):
            lanes = slice(j * LANES, (j + 1) * LANES)
            ob[part, lanes] = (u[j, part] * scale[part] * gain_v[:, lanes]).astype(BF16)
        o_copy(i).start()
    pltpu.make_async_copy(ob, out_hbm, o_sem).wait()


def solution(mesh, group=GROUP):
    n = mesh.shape["seq"]

    def local(inner, gate, proj, raw, conv_weight, conv_bias, step_bias, rate, skip, gain):
        rows, width = inner.shape
        heads = width // HEAD
        blocks = width // LANES
        per = blocks // group
        groups = n // group
        states = proj.shape[1] // 4
        taps = conv_weight.shape[1]
        dma = pltpu.SemaphoreType.DMA
        vm = pltpu.VMEM
        wide16 = vm((blocks, rows, LANES), BF16)
        wide32 = vm((blocks, rows, LANES), F32)
        scratch = [
            vm((rows, width), BF16),
            vm((rows, width), BF16),
            vm((blocks, rows + 16, LANES), F32),
            wide16,
            wide16,
            wide16,
            wide16,
            wide32,
            wide32,
            vm((2, blocks, rows, LANES), F32),
            vm((blocks, 8, LANES), F32),
            vm(proj.shape[::-1], BF16),
            vm(raw.shape[::-1], BF16),
            vm(conv_weight.shape, F32),
            vm(conv_bias.shape, F32),
            vm(step_bias.shape, F32),
            vm(rate.shape, F32),
            vm(skip.shape, F32),
            vm((4 * rows + 16, 2 * heads), BF16),
            vm((rows, rows), BF16),
            vm((rows, rows), BF16),
            vm((2, states, rows), BF16),
            vm((2, rows, states), BF16),
            vm((8, width), BF16),
            vm((8, width), BF16),
            vm((8, LANES), F32),
            vm((group, 8, LANES), F32),
            vm((8, LANES), F32),
            vm((groups, 8, LANES), F32),
            vm((group, per, 2 * states, LANES), BF16),
            vm((group, per, 2 * states, LANES), BF16),
            vm((2, per, states, LANES), BF16),
            vm((groups, per, states, LANES), BF16),
            vm((group, per, 2 * states, LANES), BF16),
            vm((group, per, 2 * states, LANES), BF16),
            dma,
            dma,
            dma((7,)),
            pltpu.SemaphoreType.REGULAR((max(1, groups // 2 - 1),)),
            dma((2,)),
            dma((2,)),
        ]
        scratch += [dma] * 9 + [dma((group - 1,))]
        vmem = pl.BlockSpec(memory_space=pltpu.VMEM)
        hbm = pl.BlockSpec(memory_space=pl.ANY)
        gated, sumsq = pl.pallas_call(
            functools.partial(kernel, n, group, heads, taps),
            out_shape=(
                jax.ShapeDtypeStruct((blocks, rows, LANES), F32),
                jax.ShapeDtypeStruct((rows, LANES), F32),
            ),
            in_specs=[hbm] * 9,
            out_specs=(vmem, vmem),
            scratch_shapes=scratch,
            compiler_params=pltpu.CompilerParams(
                collective_id=0, has_side_effects=True, vmem_limit_bytes=36 * 2**20
            ),
            name="mixer",
        )(
            *(
                pltpu.with_memory_space_constraint(array, pltpu.HBM)
                for array in (
                    inner, gate, proj.T, raw.T, conv_weight, conv_bias, step_bias, rate, skip
                )
            )
        )
        return pl.pallas_call(
            finale,
            out_shape=jax.ShapeDtypeStruct((rows, width), BF16),
            in_specs=[vmem, vmem, hbm],
            out_specs=hbm,
            scratch_shapes=[
                vm((rows, width), BF16), vm((1, width), F32), dma, dma
            ],
            compiler_params=pltpu.CompilerParams(vmem_limit_bytes=16 * 2**20),
            name="finale",
        )(gated, sumsq, gain.reshape(1, width))

    spec = P(("img", "seq"), None)
    return jax.shard_map(
        local,
        mesh=mesh,
        in_specs=(spec, spec, spec, spec, P(), P(), P(), P(), P(), P()),
        out_specs=spec,
        check_vma=False,
    )
```

```python
import functools

import jax
import jax.numpy as jnp
from jax import lax
from jax.experimental import pallas as pl
from jax.experimental.pallas import tpu as pltpu
from jax.sharding import PartitionSpec as P

MESH = pl.DeviceIdType.MESH
F32 = jnp.float32
BF16 = jnp.bfloat16
LANES = 128
HEAD = 64
GROUP = 8
NEAR = (6, 5, 7, 2, 4, 1, 3)
FAR = (4, 3, 5, 2, 6, 1, 7)
BAND = 32


def split(v):
    high = v.astype(BF16).astype(F32)
    return jnp.concatenate([high, v - high], axis=1).astype(BF16)


def spreader(block, heads, rows):
    row = lax.broadcasted_iota(jnp.int32, (rows, LANES), 0)
    lane = lax.broadcasted_iota(jnp.int32, (rows, LANES), 1)
    row = jnp.where(row >= heads, row - heads, row)
    head = 2 * block + jnp.where(lane >= HEAD, 1, 0)
    return jnp.where(row == head, 1.0, 0.0).astype(BF16)


def dot(a, b):
    return jnp.dot(a, b, preferred_element_type=F32)


def silu(v):
    half = 0.5 * v
    return half + half * jnp.tanh(half)


def kernel(
    n, group, heads, kernel_taps,
    x_hbm, gate_hbm, proj_hbm, raw_hbm, cw_hbm, cb_hbm, sb_hbm, rate_hbm, skip_hbm,
    u, sumsq,
    xb, gb, xs, cf, cr, gf, gr, ef, er, gw, ext,
    proj_v, raw_v, cw_v, cb_v, sb_v, rate_v, skip_v,
    lhs, mf, mr, bt, cm,
    prev_v, next_v, tot_v, tots_v, totg_v, totr_v,
    send1, recv1, send2, recv2, send3, recv3,
    x_sem, g_sem, s_sem, ready, h_send, h_recv,
    t1_send, t1_recv, t2_send, t2_recv, c1_send, c1_recv, c2_send, c2_recv, c3_send, c3_recv,
):
    rows = u.shape[1]
    blocks = u.shape[0]
    per = blocks // group
    groups = n // group
    states = bt.shape[1]
    me = lax.axis_index("seq")
    mem = lax.rem(me, group)
    grp = lax.div(me, group)
    base = me - mem

    def lanes(j):
        return pl.ds(pl.multiple_of(j * LANES, LANES), LANES)

    def pick(table, r):
        found = 0
        for k, value in enumerate(table):
            found = found + jnp.where(r == k + 1, value, 0)
        return found

    def offset(r, way):
        if group != 8:
            return lax.rem(mem + way * r + group, group)
        code = pick(NEAR, r)
        across = lax.rem(lax.div(mem, 4) + lax.div(code, 4), 2)
        return across * 4 + lax.rem(lax.rem(mem, 4) + way * lax.rem(code, 4) + 4, 4)

    def member(r):
        return offset(r, 1)

    def far(r):
        return lax.rem(grp + (pick(FAR, r) if groups == 8 else r), groups)

    def sweep(body, many):
        def turn(i, carry):
            for q in range(many):
                body(i * many + q)
            return carry

        lax.fori_loop(0, blocks // many, turn, 0)

    small = [
        (raw_hbm, raw_v), (sb_hbm, sb_v), (rate_hbm, rate_v), (proj_hbm, proj_v),
        (skip_hbm, skip_v), (cw_hbm, cw_v), (cb_hbm, cb_v),
    ]
    loads = [pltpu.make_async_copy(a, b, s_sem.at[i]) for i, (a, b) in enumerate(small)]
    for copy in loads:
        copy.start()

    bands = rows // BAND

    def x_copy(i):
        band = pl.ds(i * BAND, BAND)
        return pltpu.make_async_copy(x_hbm.at[band], xb.at[band], x_sem)

    def g_copy(i):
        band = pl.ds(i * BAND, BAND)
        return pltpu.make_async_copy(gate_hbm.at[band], gb.at[band], g_sem)

    for i in range(bands):
        x_copy(i).start()

    barrier = pltpu.get_barrier_semaphore()
    after = lax.rem(me + 1, n)
    before = lax.rem(me + n - 1, n)
    beside = (lax.rem(me + group, n), lax.rem(me + n - group, n))

    def signal(semaphore, peer):
        pl.semaphore_signal(semaphore, inc=1, device_id={"seq": peer}, device_id_type=MESH)

    for peer in (after, before) + beside:
        signal(barrier, peer)
    for r in range(1, group):
        signal(barrier, base + member(r))

    for i in range(bands):
        g_copy(i).start()

    pl.semaphore_wait(barrier, 4 + (group - 1))
    edge = 8
    halo = [
        pltpu.make_async_remote_copy(
            src_ref=x_hbm.at[pl.ds(rows - edge, edge)], dst_ref=prev_v,
            send_sem=h_send.at[0], recv_sem=h_recv.at[0],
            device_id={"seq": after}, device_id_type=MESH,
        ),
        pltpu.make_async_remote_copy(
            src_ref=x_hbm.at[pl.ds(0, edge)], dst_ref=next_v,
            send_sem=h_send.at[1], recv_sem=h_recv.at[1],
            device_id={"seq": before}, device_id_type=MESH,
        ),
    ]
    for copy in halo:
        copy.start()
    rounds = groups // 2 - 1

    def relay(k):
        if 0 < k <= rounds:
            pl.semaphore_wait(ready.at[k - 1], 2)
        if k < rounds:
            for peer in beside:
                signal(ready.at[k], peer)

    relay(0)
    for copy in loads[:5]:
        copy.wait()

    first_t = lax.broadcasted_iota(jnp.int32, (rows, rows), 0)
    second_t = lax.broadcasted_iota(jnp.int32, (rows, rows), 1)
    masks = (first_t >= second_t, first_t <= second_t)
    lasts = (rows - 1, 0)
    raw = raw_v[...].astype(F32)
    params = jnp.concatenate(
        [
            jnp.concatenate([sb_v[...], rate_v[...], jnp.zeros((4, heads), F32)], axis=0),
            jnp.zeros((8, LANES - heads), F32),
        ],
        axis=1,
    ).T
    zeros = jnp.zeros((16 - 4, heads), F32)
    grow, decay, total, skips = [], [], [], []
    for d in range(2):
        v = raw[d * heads : (d + 1) * heads] + params[:heads, d : d + 1]
        step = jnp.maximum(v, 0.0) + jnp.log1p(jnp.exp(-jnp.abs(v)))
        cumul = jnp.dot(
            -params[:heads, 2 + d : 3 + d] * step,
            jnp.where(masks[1 - d], 1.0, 0.0),
            precision=lax.Precision.HIGHEST,
            preferred_element_type=F32,
        )
        grow.append((jnp.exp(-cumul) * step).T)
        decay.append(jnp.exp(cumul).T)
        total.append(decay[d][lasts[d] : lasts[d] + 1, :])
        skips.append(skip_v[d : d + 1, :])
        first = 2 * d * states
        write_t = proj_v[first : first + states, :]
        read = proj_v[first + states : first + 2 * states, :].astype(F32).T.astype(BF16)
        bt[d] = write_t
        cm[d] = read
        scores = jnp.where(masks[d], dot(read, write_t), 0.0).astype(BF16)
        (mf, mr)[d][...] = scores
    lhs[...] = split(jnp.concatenate(decay + grow + total + skips + [zeros], axis=0))
    tot_v[...] = jnp.concatenate(
        [
            jnp.concatenate(total, axis=0),
            jnp.zeros((2, LANES - heads), F32),
        ],
        axis=1,
    )

    def near_copy(src, dst, ss, rs, r):
        return pltpu.make_async_remote_copy(
            src_ref=src, dst_ref=dst, send_sem=ss, recv_sem=rs,
            device_id={"seq": base + member(r)}, device_id_type=MESH,
        )

    def far_copy(src, dst, ss, rs, r):
        return pltpu.make_async_remote_copy(
            src_ref=src, dst_ref=dst, send_sem=ss, recv_sem=rs,
            device_id={"seq": far(r) * group + mem}, device_id_type=MESH,
        )

    def t1(r):
        return near_copy(tot_v, tots_v.at[mem], t1_send, t1_recv, r)

    def t2(r):
        return far_copy(totg_v, totr_v.at[grp], t2_send, t2_recv, r)

    def c1(r):
        return near_copy(send1.at[member(r)], recv1.at[mem], c1_send, c1_recv, r)

    def c2(r, b):
        ahead = jnp.where(far(r) > grp, 0, 1)
        return far_copy(
            send2.at[ahead, b], recv2.at[b, grp], c2_send.at[b], c2_recv.at[b], r
        )

    def c3(r, b):
        return near_copy(
            send3.at[b, member(r)], recv3.at[b, mem], c3_send.at[b], c3_recv.at[b], r
        )

    near_all, far_all = pl.ds(0, group - 1), pl.ds(0, groups - 1)
    t1_all = near_copy(tots_v.at[near_all], tots_v.at[near_all], t1_send, t1_recv, 1)
    t2_all = far_copy(totr_v.at[far_all], totr_v.at[far_all], t2_send, t2_recv, 1)
    c1_all = near_copy(send1.at[near_all], recv1.at[near_all], c1_send, c1_recv, 1)

    def c2_all(b):
        whole = recv2.at[b, far_all]
        return far_copy(whole, whole, c2_send.at[b], c2_recv.at[b], 1)

    def c3_all(b):
        return near_copy(
            send3.at[b, near_all], recv3.at[b, near_all], c3_send.at[b], c3_recv.at[b], 1
        )


    def loop(first, last, action):
        def body(r, carry):
            action(r)
            return carry

        lax.fori_loop(first, last, body, 0)

    loop(1, group, lambda r: t1(r).start())
    tots_v[mem] = tot_v[...]

    def growth(j):
        wide = dot(lhs[pl.ds(2 * rows, 2 * rows + 16), :], spreader(j, heads, 2 * heads))
        gw[0, j] = wide[:rows]
        gw[1, j] = wide[rows : 2 * rows]
        ext[j] = wide[2 * rows : 2 * rows + 8]

    sweep(growth, 3)
    relay(1)
    for copy in loads[5:]:
        copy.wait()
    pltpu.make_async_copy(x_hbm, xb, x_sem).wait()
    for copy in halo:
        copy.wait()

    has_before = jnp.where(me > 0, 1.0, 0.0)
    has_after = jnp.where(me < n - 1, 1.0, 0.0)

    def conv(owner):
        for b in range(per):
            j = owner * per + b
            xs[j, pl.ds(0, 8), :] = prev_v[:, lanes(j)].astype(F32) * has_before
            xs[j, pl.ds(8 + rows, 8), :] = next_v[:, lanes(j)].astype(F32) * has_after
            xs[j, pl.ds(8, rows), :] = xb[:, lanes(j)].astype(F32)
        for b in range(per):
            j = owner * per + b
            for d in range(2):
                acc = 0.5 * cb_v[d : d + 1, lanes(j)]
                for k in range(kernel_taps):
                    shift = -k if d == 0 else k
                    tap = 0.5 * cw_v[d, k : k + 1, lanes(j)]
                    acc = acc + tap * xs[j, pl.ds(8 + shift, rows), :]
                conved = (acc + acc * jnp.tanh(acc)).astype(BF16)
                (cf, cr)[d][j] = conved
                (gf, gr)[d][j] = (gw[d, j] * conved.astype(F32)).astype(BF16)

    def finish(owner, buffer):
        results = []
        for b in range(per):
            j = owner * per + b
            for d in range(2):
                end = dot(bt[d], (gf, gr)[d][j]) * ext[j, pl.ds(d, 1), :]
                results.append((b, d, end.astype(BF16)))
        for b, d, end in results:
            buffer[owner, b, pl.ds(d * states, states), :] = end

    conv(member(1))

    def ends(r):
        finish(member(r), send1)
        conv(member(r + 1))
        c1(r).start()

    loop(1, group, ends)
    finish(mem, recv1)
    relay(2)

    t1_all.wait()
    product = tots_v[0]
    for m in range(1, group):
        product = product * tots_v[m]
    totg_v[...] = product
    totr_v[grp] = product
    pltpu.make_async_copy(gate_hbm, gb, g_sem).wait()

    def inner(j):
        wide = dot(lhs[pl.ds(0, 2 * rows), :], spreader(j, heads, 2 * heads))
        gate = silu(gb[:, lanes(j)].astype(F32))
        far_f, far_r = wide[:rows] * gate, wide[rows:] * gate
        ef[j] = far_f
        er[j] = far_r
        direct = (
            ext[j, pl.ds(2, 1), :] * cf[j].astype(F32) + ext[j, pl.ds(3, 1), :] * cr[j].astype(F32)
        )
        u[j] = direct * gate + far_f * dot(mf[...], gf[j]) + far_r * dot(mr[...], gr[j])

    sweep(inner, 3)
    relay(3)
    loop(1, groups, lambda r: t2(r).start())

    c1_all.wait_recv()

    def spread(values, b):
        flat = values[...].reshape(-1, LANES)
        high = flat.astype(BF16)
        low = (flat - high.astype(F32)).astype(BF16)
        ones = spreader(mem * per + b, LANES, LANES)
        return dot(high, ones) + dot(low, ones)

    near_t = [spread(tots_v, b) for b in range(per)]

    def part(ref, m, b, d):
        return ref[m, b, pl.ds(d * states, states), :].astype(F32)

    for b in range(per):
        run_f = jnp.zeros((states, LANES), F32)
        run_r = jnp.zeros((states, LANES), F32)
        for m in range(group):
            run_f = run_f * near_t[b][2 * m : 2 * m + 1] + part(recv1, m, b, 0)
            k = group - 1 - m
            run_r = run_r * near_t[b][2 * k + 1 : 2 * k + 2] + part(recv1, k, b, 1)
        send2[0, b] = run_f.astype(BF16)
        send2[1, b] = run_r.astype(BF16)
        loop(1, groups, lambda r: c2(r, b).start())
    t2_all.wait()
    far_t = [spread(totr_v, b) for b in range(per)]
    for b in range(per):
        recv2[b, grp] = send2[0, b]

    for b in range(per):
        c2_all(b).wait_recv()
        run_f = jnp.zeros((states, LANES), F32)
        run_r = jnp.zeros((states, LANES), F32)
        for g in range(groups):
            new = run_f * far_t[b][2 * g : 2 * g + 1] + recv2[b, g].astype(F32)
            run_f = jnp.where(g < grp, new, run_f)
            k = groups - 1 - g
            new = run_r * far_t[b][2 * k + 1 : 2 * k + 2] + recv2[b, k].astype(F32)
            run_r = jnp.where(k > grp, new, run_r)
        for m in range(group):
            send3[b, m, pl.ds(0, states), :] = run_f.astype(BF16)
            run_f = run_f * near_t[b][2 * m : 2 * m + 1] + part(recv1, m, b, 0)
            k = group - 1 - m
            send3[b, k, pl.ds(states, states), :] = run_r.astype(BF16)
            run_r = run_r * near_t[b][2 * k + 1 : 2 * k + 2] + part(recv1, k, b, 1)
        loop(1, group, lambda r: c3(r, b).start())
        recv3[b, mem] = send3[b, mem]

    sumsq[...] = jnp.zeros_like(sumsq)
    many = min(4, group)
    for b in range(per):
        c3_all(b).wait_recv()

        def outer(i, carry):
            squares = jnp.zeros((rows, LANES), F32)
            for q in range(many):
                owner = i * many + q
                j = owner * per + b
                gated = (
                    u[j]
                    + ef[j] * dot(cm[0], recv3[b, owner, pl.ds(0, states), :])
                    + er[j] * dot(cm[1], recv3[b, owner, pl.ds(states, states), :])
                )
                u[j] = gated
                squares = squares + gated * gated
            sumsq[...] += squares
            return carry

        lax.fori_loop(0, group // many, outer, 0)

    c1_all.wait_send()
    for b in range(per):
        c2_all(b).wait_send()
        c3_all(b).wait_send()


def finale(u, sumsq, gain_hbm, out_hbm, ob, gain_v, o_sem, s_sem):
    blocks, rows, _ = u.shape
    load = pltpu.make_async_copy(gain_hbm, gain_v, s_sem)
    load.start()
    mean = jnp.sum(sumsq[...], axis=1, keepdims=True) * (1.0 / (blocks * LANES))
    scale = lax.rsqrt(mean + 1e-05)
    load.wait()

    def o_copy(i):
        band = pl.ds(i * BAND, BAND)
        return pltpu.make_async_copy(ob.at[band], out_hbm.at[band], o_sem)

    for i in range(rows // BAND):
        part = slice(i * BAND, (i + 1) * BAND)
        for j in range(blocks):
            lanes = slice(j * LANES, (j + 1) * LANES)
            ob[part, lanes] = (u[j, part] * scale[part] * gain_v[:, lanes]).astype(BF16)
        o_copy(i).start()
    pltpu.make_async_copy(ob, out_hbm, o_sem).wait()


def solution(mesh, group=GROUP):
    n = mesh.shape["seq"]

    def local(inner, gate, proj, raw, conv_weight, conv_bias, step_bias, rate, skip, gain):
        rows, width = inner.shape
        heads = width // HEAD
        blocks = width // LANES
        per = blocks // group
        groups = n // group
        states = proj.shape[1] // 4
        taps = conv_weight.shape[1]
        dma = pltpu.SemaphoreType.DMA
        vm = pltpu.VMEM
        wide16 = vm((blocks, rows, LANES), BF16)
        wide32 = vm((blocks, rows, LANES), F32)
        scratch = [
            vm((rows, width), BF16),
            vm((rows, width), BF16),
            vm((blocks, rows + 16, LANES), F32),
            wide16,
            wide16,
            wide16,
            wide16,
            wide32,
            wide32,
            vm((2, blocks, rows, LANES), F32),
            vm((blocks, 8, LANES), F32),
            vm(proj.shape[::-1], BF16),
            vm(raw.shape[::-1], BF16),
            vm(conv_weight.shape, F32),
            vm(conv_bias.shape, F32),
            vm(step_bias.shape, F32),
            vm(rate.shape, F32),
            vm(skip.shape, F32),
            vm((4 * rows + 16, 2 * heads), BF16),
            vm((rows, rows), BF16),
            vm((rows, rows), BF16),
            vm((2, states, rows), BF16),
            vm((2, rows, states), BF16),
            vm((8, width), BF16),
            vm((8, width), BF16),
            vm((2, LANES), F32),
            vm((group, 2, LANES), F32),
            vm((2, LANES), F32),
            vm((groups, 2, LANES), F32),
            vm((group, per, 2 * states, LANES), BF16),
            vm((group, per, 2 * states, LANES), BF16),
            vm((2, per, states, LANES), BF16),
            vm((per, groups, states, LANES), BF16),
            vm((per, group, 2 * states, LANES), BF16),
            vm((per, group, 2 * states, LANES), BF16),
            dma,
            dma,
            dma((7,)),
            pltpu.SemaphoreType.REGULAR((max(1, groups // 2 - 1),)),
            dma((2,)),
            dma((2,)),
        ]
        scratch += [dma] * 6 + [dma((per,))] * 4
        vmem = pl.BlockSpec(memory_space=pltpu.VMEM)
        hbm = pl.BlockSpec(memory_space=pl.ANY)
        gated, sumsq = pl.pallas_call(
            functools.partial(kernel, n, group, heads, taps),
            out_shape=(
                jax.ShapeDtypeStruct((blocks, rows, LANES), F32),
                jax.ShapeDtypeStruct((rows, LANES), F32),
            ),
            in_specs=[hbm] * 9,
            out_specs=(vmem, vmem),
            scratch_shapes=scratch,
            compiler_params=pltpu.CompilerParams(
                collective_id=0, has_side_effects=True, vmem_limit_bytes=36 * 2**20
            ),
            name="mixer",
        )(
            *(
                pltpu.with_memory_space_constraint(array, pltpu.HBM)
                for array in (
                    inner, gate, proj.T, raw.T, conv_weight, conv_bias, step_bias, rate, skip
                )
            )
        )
        return pl.pallas_call(
            finale,
            out_shape=jax.ShapeDtypeStruct((rows, width), BF16),
            in_specs=[vmem, vmem, hbm],
            out_specs=hbm,
            scratch_shapes=[
                vm((rows, width), BF16), vm((1, width), F32), dma, dma
            ],
            compiler_params=pltpu.CompilerParams(vmem_limit_bytes=16 * 2**20),
            name="finale",
        )(gated, sumsq, gain.reshape(1, width))

    spec = P(("img", "seq"), None)
    return jax.shard_map(
        local,
        mesh=mesh,
        in_specs=(spec, spec, spec, spec, P(), P(), P(), P(), P(), P()),
        out_specs=spec,
        check_vma=False,
    )
```

```python
import functools

import jax
import jax.numpy as jnp
from jax import lax
from jax.experimental import pallas as pl
from jax.experimental.pallas import tpu as pltpu
from jax.sharding import PartitionSpec as P

MESH = pl.DeviceIdType.MESH
F32 = jnp.float32
BF16 = jnp.bfloat16
LANES = 128
HEAD = 64
GROUP = 8
NEAR = (6, 5, 7, 2, 4, 1, 3)
FAR = (4, 3, 5, 2, 6, 1, 7)
BAND = 32


def split(v):
    high = v.astype(BF16).astype(F32)
    return jnp.concatenate([high, v - high], axis=1).astype(BF16)


def spreader(block, heads, rows):
    row = lax.broadcasted_iota(jnp.int32, (rows, LANES), 0)
    lane = lax.broadcasted_iota(jnp.int32, (rows, LANES), 1)
    row = jnp.where(row >= heads, row - heads, row)
    head = 2 * block + jnp.where(lane >= HEAD, 1, 0)
    return jnp.where(row == head, 1.0, 0.0).astype(BF16)


def dot(a, b):
    return jnp.dot(a, b, preferred_element_type=F32)


def silu(v):
    half = 0.5 * v
    return half + half * jnp.tanh(half)


def kernel(
    n, group, heads, kernel_taps,
    x_hbm, gate_hbm, proj_hbm, raw_hbm, cw_hbm, cb_hbm, sb_hbm, rate_hbm, skip_hbm,
    u, sumsq,
    xb, gb, xs, cf, cr, gf, gr, ef, er, gw, ext,
    proj_v, raw_v, cw_v, cb_v, sb_v, rate_v, skip_v,
    lhs, mf, mr, bt, cm,
    prev_v, next_v, tot_v, tots_v, totg_v, totr_v,
    send1, recv1, send2, recv2, send3, recv3,
    x_sem, g_sem, s_sem, ready, h_send, h_recv,
    t1_send, t1_recv, t2_send, t2_recv, c1_send, c1_recv, c2_send, c2_recv, c3_send, c3_recv,
):
    rows = u.shape[1]
    blocks = u.shape[0]
    per = blocks // group
    groups = n // group
    states = bt.shape[1]
    me = lax.axis_index("seq")
    mem = lax.rem(me, group)
    grp = lax.div(me, group)
    base = me - mem

    def lanes(j):
        return pl.ds(pl.multiple_of(j * LANES, LANES), LANES)

    def pick(table, r):
        if isinstance(r, int):
            return table[r - 1]
        found = 0
        for k, value in enumerate(table):
            found = found + jnp.where(r == k + 1, value, 0)
        return found

    def offset(r, way):
        if group != 8:
            return lax.rem(mem + way * r + group, group)
        code = pick(NEAR, r)
        high, low = (divmod(code, 4)) if isinstance(code, int) else (lax.div(code, 4), lax.rem(code, 4))
        across = lax.rem(lax.div(mem, 4) + high, 2)
        return across * 4 + lax.rem(lax.rem(mem, 4) + way * low + 4, 4)

    def member(r):
        return offset(r, 1)

    def far(r):
        return lax.rem(grp + (pick(FAR, r) if groups == 8 else r), groups)

    def sweep(body, many):
        def turn(i, carry):
            for q in range(many):
                body(i * many + q)
            return carry

        lax.fori_loop(0, blocks // many, turn, 0)

    small = [
        (raw_hbm, raw_v), (sb_hbm, sb_v), (rate_hbm, rate_v), (proj_hbm, proj_v),
        (skip_hbm, skip_v), (cw_hbm, cw_v), (cb_hbm, cb_v),
    ]
    loads = [pltpu.make_async_copy(a, b, s_sem.at[i]) for i, (a, b) in enumerate(small)]
    for copy in loads:
        copy.start()

    bands = rows // BAND

    def x_copy(i):
        band = pl.ds(i * BAND, BAND)
        return pltpu.make_async_copy(x_hbm.at[band], xb.at[band], x_sem)

    def g_copy(i):
        band = pl.ds(i * BAND, BAND)
        return pltpu.make_async_copy(gate_hbm.at[band], gb.at[band], g_sem)

    for i in range(bands):
        x_copy(i).start()

    barrier = pltpu.get_barrier_semaphore()
    after = lax.rem(me + 1, n)
    before = lax.rem(me + n - 1, n)
    beside = (lax.rem(me + group, n), lax.rem(me + n - group, n))

    def signal(semaphore, peer):
        pl.semaphore_signal(semaphore, inc=1, device_id={"seq": peer}, device_id_type=MESH)

    for peer in (after, before) + beside:
        signal(barrier, peer)
    for r in range(1, group):
        signal(barrier, base + member(r))

    for i in range(bands):
        g_copy(i).start()

    pl.semaphore_wait(barrier, 4 + (group - 1))
    edge = 8
    halo = [
        pltpu.make_async_remote_copy(
            src_ref=x_hbm.at[pl.ds(rows - edge, edge)], dst_ref=prev_v,
            send_sem=h_send.at[0], recv_sem=h_recv.at[0],
            device_id={"seq": after}, device_id_type=MESH,
        ),
        pltpu.make_async_remote_copy(
            src_ref=x_hbm.at[pl.ds(0, edge)], dst_ref=next_v,
            send_sem=h_send.at[1], recv_sem=h_recv.at[1],
            device_id={"seq": before}, device_id_type=MESH,
        ),
    ]
    for copy in halo:
        copy.start()
    rounds = groups // 2 - 1

    def relay(k):
        if 0 < k <= rounds:
            pl.semaphore_wait(ready.at[k - 1], 2)
        if k < rounds:
            for peer in beside:
                signal(ready.at[k], peer)

    relay(0)
    first_t = lax.broadcasted_iota(jnp.int32, (rows, rows), 0)
    second_t = lax.broadcasted_iota(jnp.int32, (rows, rows), 1)
    masks = (first_t >= second_t, first_t <= second_t)
    for copy in loads[:5]:
        copy.wait()

    lasts = (rows - 1, 0)
    raw = raw_v[...].astype(F32)
    params = jnp.concatenate(
        [
            jnp.concatenate([sb_v[...], rate_v[...], jnp.zeros((4, heads), F32)], axis=0),
            jnp.zeros((8, LANES - heads), F32),
        ],
        axis=1,
    ).T
    zeros = jnp.zeros((16 - 4, heads), F32)
    grow, decay, total, skips = [], [], [], []
    for d in range(2):
        v = raw[d * heads : (d + 1) * heads] + params[:heads, d : d + 1]
        step = jnp.maximum(v, 0.0) + jnp.log1p(jnp.exp(-jnp.abs(v)))
        cumul = jnp.dot(
            -params[:heads, 2 + d : 3 + d] * step,
            jnp.where(masks[1 - d], 1.0, 0.0),
            precision=lax.Precision.HIGHEST,
            preferred_element_type=F32,
        )
        grow.append((jnp.exp(-cumul) * step).T)
        decay.append(jnp.exp(cumul).T)
        total.append(decay[d][lasts[d] : lasts[d] + 1, :])
        skips.append(skip_v[d : d + 1, :])
        first = 2 * d * states
        write_t = proj_v[first : first + states, :]
        read = proj_v[first + states : first + 2 * states, :].astype(F32).T.astype(BF16)
        bt[d] = write_t
        cm[d] = read
        scores = jnp.where(masks[d], dot(read, write_t), 0.0).astype(BF16)
        (mf, mr)[d][...] = scores
    lhs[...] = split(jnp.concatenate(decay + grow + total + skips + [zeros], axis=0))
    tot_v[...] = jnp.concatenate(
        [
            jnp.concatenate(total, axis=0),
            jnp.zeros((2, LANES - heads), F32),
        ],
        axis=1,
    )

    def near_copy(src, dst, ss, rs, r):
        return pltpu.make_async_remote_copy(
            src_ref=src, dst_ref=dst, send_sem=ss, recv_sem=rs,
            device_id={"seq": base + member(r)}, device_id_type=MESH,
        )

    def far_copy(src, dst, ss, rs, r):
        return pltpu.make_async_remote_copy(
            src_ref=src, dst_ref=dst, send_sem=ss, recv_sem=rs,
            device_id={"seq": far(r) * group + mem}, device_id_type=MESH,
        )

    def t1(r):
        return near_copy(tot_v, tots_v.at[mem], t1_send, t1_recv, r)

    def t2(r):
        return far_copy(totg_v, totr_v.at[grp], t2_send, t2_recv, r)

    def c1(r):
        return near_copy(send1.at[member(r)], recv1.at[mem], c1_send, c1_recv, r)

    def c2(r, b):
        ahead = jnp.where(far(r) > grp, 0, 1)
        return far_copy(
            send2.at[ahead, b], recv2.at[b, grp], c2_send.at[b], c2_recv.at[b], r
        )

    def c3(r, b):
        return near_copy(
            send3.at[b, member(r)], recv3.at[b, mem], c3_send.at[b], c3_recv.at[b], r
        )

    near_all, far_all = pl.ds(0, group - 1), pl.ds(0, groups - 1)
    t1_all = near_copy(tots_v.at[near_all], tots_v.at[near_all], t1_send, t1_recv, 1)
    t2_all = far_copy(totr_v.at[far_all], totr_v.at[far_all], t2_send, t2_recv, 1)
    c1_all = near_copy(send1.at[near_all], recv1.at[near_all], c1_send, c1_recv, 1)

    def c2_all(b):
        whole = recv2.at[b, far_all]
        return far_copy(whole, whole, c2_send.at[b], c2_recv.at[b], 1)

    def c3_all(b):
        return near_copy(
            send3.at[b, near_all], recv3.at[b, near_all], c3_send.at[b], c3_recv.at[b], 1
        )


    def loop(first, last, action):
        def body(r, carry):
            action(r)
            return carry

        lax.fori_loop(first, last, body, 0)

    for r in range(1, group):
        t1(r).start()
    tots_v[mem] = tot_v[...]

    def growth(j):
        wide = dot(lhs[pl.ds(2 * rows, 2 * rows + 16), :], spreader(j, heads, 2 * heads))
        gw[0, j] = wide[:rows]
        gw[1, j] = wide[rows : 2 * rows]
        ext[j] = wide[2 * rows : 2 * rows + 8]

    sweep(growth, 12)
    relay(1)
    for copy in loads[5:]:
        copy.wait()
    pltpu.make_async_copy(x_hbm, xb, x_sem).wait()
    for copy in halo:
        copy.wait()

    has_before = jnp.where(me > 0, 1.0, 0.0)
    has_after = jnp.where(me < n - 1, 1.0, 0.0)

    def conv(owner):
        for b in range(per):
            j = owner * per + b
            xs[j, pl.ds(0, 8), :] = prev_v[:, lanes(j)].astype(F32) * has_before
            xs[j, pl.ds(8 + rows, 8), :] = next_v[:, lanes(j)].astype(F32) * has_after
            xs[j, pl.ds(8, rows), :] = xb[:, lanes(j)].astype(F32)
        for b in range(per):
            j = owner * per + b
            for d in range(2):
                acc = 0.5 * cb_v[d : d + 1, lanes(j)]
                for k in range(kernel_taps):
                    shift = -k if d == 0 else k
                    tap = 0.5 * cw_v[d, k : k + 1, lanes(j)]
                    acc = acc + tap * xs[j, pl.ds(8 + shift, rows), :]
                conved = (acc + acc * jnp.tanh(acc)).astype(BF16)
                (cf, cr)[d][j] = conved
                (gf, gr)[d][j] = (gw[d, j] * conved.astype(F32)).astype(BF16)

    def finish(owner, buffer):
        results = []
        for b in range(per):
            j = owner * per + b
            for d in range(2):
                end = dot(bt[d], (gf, gr)[d][j]) * ext[j, pl.ds(d, 1), :]
                results.append((b, d, end.astype(BF16)))
        for b, d, end in results:
            buffer[owner, b, pl.ds(d * states, states), :] = end

    conv(member(1))

    def ends(r):
        finish(member(r), send1)
        conv(member(r + 1))
        c1(r).start()

    loop(1, group, ends)
    finish(mem, recv1)
    relay(2)

    t1_all.wait()
    product = tots_v[0]
    for m in range(1, group):
        product = product * tots_v[m]
    totg_v[...] = product
    totr_v[grp] = product
    pltpu.make_async_copy(gate_hbm, gb, g_sem).wait()

    def inner(j):
        wide = dot(lhs[pl.ds(0, 2 * rows), :], spreader(j, heads, 2 * heads))
        gate = silu(gb[:, lanes(j)].astype(F32))
        far_f, far_r = wide[:rows] * gate, wide[rows:] * gate
        ef[j] = far_f
        er[j] = far_r
        direct = (
            ext[j, pl.ds(2, 1), :] * cf[j].astype(F32) + ext[j, pl.ds(3, 1), :] * cr[j].astype(F32)
        )
        u[j] = direct * gate + far_f * dot(mf[...], gf[j]) + far_r * dot(mr[...], gr[j])

    sweep(inner, 4)
    relay(3)
    for r in range(1, groups):
        t2(r).start()

    c1_all.wait_recv()

    def spread(values, b):
        flat = values[...].reshape(-1, LANES)
        high = flat.astype(BF16)
        low = (flat - high.astype(F32)).astype(BF16)
        ones = spreader(mem * per + b, LANES, LANES)
        return dot(high, ones) + dot(low, ones)

    near_t = [spread(tots_v, b) for b in range(per)]

    def part(ref, m, b, d):
        return ref[m, b, pl.ds(d * states, states), :].astype(F32)

    for b in range(per):
        run_f = jnp.zeros((states, LANES), F32)
        run_r = jnp.zeros((states, LANES), F32)
        for m in range(group):
            run_f = run_f * near_t[b][2 * m : 2 * m + 1] + part(recv1, m, b, 0)
            k = group - 1 - m
            run_r = run_r * near_t[b][2 * k + 1 : 2 * k + 2] + part(recv1, k, b, 1)
        send2[0, b] = run_f.astype(BF16)
        send2[1, b] = run_r.astype(BF16)
        for r in range(1, groups):
            c2(r, b).start()
    t2_all.wait()
    far_t = [spread(totr_v, b) for b in range(per)]
    for b in range(per):
        recv2[b, grp] = send2[0, b]

    for b in range(per):
        c2_all(b).wait_recv()
        run_f = jnp.zeros((states, LANES), F32)
        run_r = jnp.zeros((states, LANES), F32)
        for g in range(groups):
            new = run_f * far_t[b][2 * g : 2 * g + 1] + recv2[b, g].astype(F32)
            run_f = jnp.where(g < grp, new, run_f)
            k = groups - 1 - g
            new = run_r * far_t[b][2 * k + 1 : 2 * k + 2] + recv2[b, k].astype(F32)
            run_r = jnp.where(k > grp, new, run_r)
        for m in range(group):
            send3[b, m, pl.ds(0, states), :] = run_f.astype(BF16)
            run_f = run_f * near_t[b][2 * m : 2 * m + 1] + part(recv1, m, b, 0)
            k = group - 1 - m
            send3[b, k, pl.ds(states, states), :] = run_r.astype(BF16)
            run_r = run_r * near_t[b][2 * k + 1 : 2 * k + 2] + part(recv1, k, b, 1)
        for r in range(1, group):
            c3(r, b).start()
        recv3[b, mem] = send3[b, mem]

    sumsq[...] = jnp.zeros_like(sumsq)
    many = min(4, group)
    for b in range(per):
        c3_all(b).wait_recv()

        def outer(i, carry):
            squares = jnp.zeros((rows, LANES), F32)
            for q in range(many):
                owner = i * many + q
                j = owner * per + b
                gated = (
                    u[j]
                    + ef[j] * dot(cm[0], recv3[b, owner, pl.ds(0, states), :])
                    + er[j] * dot(cm[1], recv3[b, owner, pl.ds(states, states), :])
                )
                u[j] = gated
                squares = squares + gated * gated
            sumsq[...] += squares
            return carry

        lax.fori_loop(0, group // many, outer, 0)

    c1_all.wait_send()
    for b in range(per):
        c2_all(b).wait_send()
        c3_all(b).wait_send()


def finale(u, sumsq, gain, out_hbm, ob, o_sem):
    blocks, rows, _ = u.shape
    mean = jnp.sum(sumsq[...], axis=1, keepdims=True) * (1.0 / (blocks * LANES))
    scale = lax.rsqrt(mean + 1e-05)
    for i in range(rows // 16):
        part = slice(i * 16, (i + 1) * 16)
        for j in range(blocks):
            lanes = slice(j * LANES, (j + 1) * LANES)
            ob[part, lanes] = (u[j, part] * scale[part] * gain[:, lanes]).astype(BF16)
        band = pl.ds(i * 16, 16)
        pltpu.make_async_copy(ob.at[band], out_hbm.at[band], o_sem).start()
    pltpu.make_async_copy(ob, out_hbm, o_sem).wait()


def solution(mesh, group=GROUP):
    n = mesh.shape["seq"]

    def local(inner, gate, proj, raw, conv_weight, conv_bias, step_bias, rate, skip, gain):
        rows, width = inner.shape
        heads = width // HEAD
        blocks = width // LANES
        per = blocks // group
        groups = n // group
        states = proj.shape[1] // 4
        taps = conv_weight.shape[1]
        dma = pltpu.SemaphoreType.DMA
        vm = pltpu.VMEM
        wide16 = vm((blocks, rows, LANES), BF16)
        wide32 = vm((blocks, rows, LANES), F32)
        scratch = [
            vm((rows, width), BF16),
            vm((rows, width), BF16),
            vm((blocks, rows + 16, LANES), F32),
            wide16,
            wide16,
            wide16,
            wide16,
            wide32,
            wide32,
            vm((2, blocks, rows, LANES), F32),
            vm((blocks, 8, LANES), F32),
            vm(proj.shape[::-1], BF16),
            vm(raw.shape[::-1], BF16),
            vm(conv_weight.shape, F32),
            vm(conv_bias.shape, F32),
            vm(step_bias.shape, F32),
            vm(rate.shape, F32),
            vm(skip.shape, F32),
            vm((4 * rows + 16, 2 * heads), BF16),
            vm((rows, rows), BF16),
            vm((rows, rows), BF16),
            vm((2, states, rows), BF16),
            vm((2, rows, states), BF16),
            vm((8, width), BF16),
            vm((8, width), BF16),
            vm((2, LANES), F32),
            vm((group, 2, LANES), F32),
            vm((2, LANES), F32),
            vm((groups, 2, LANES), F32),
            vm((group, per, 2 * states, LANES), BF16),
            vm((group, per, 2 * states, LANES), BF16),
            vm((2, per, states, LANES), BF16),
            vm((per, groups, states, LANES), BF16),
            vm((per, group, 2 * states, LANES), BF16),
            vm((per, group, 2 * states, LANES), BF16),
            dma,
            dma,
            dma((7,)),
            pltpu.SemaphoreType.REGULAR((max(1, groups // 2 - 1),)),
            dma((2,)),
            dma((2,)),
        ]
        scratch += [dma] * 6 + [dma((per,))] * 4
        vmem = pl.BlockSpec(memory_space=pltpu.VMEM)
        hbm = pl.BlockSpec(memory_space=pl.ANY)
        gated, sumsq = pl.pallas_call(
            functools.partial(kernel, n, group, heads, taps),
            out_shape=(
                jax.ShapeDtypeStruct((blocks, rows, LANES), F32),
                jax.ShapeDtypeStruct((rows, LANES), F32),
            ),
            in_specs=[hbm] * 9,
            out_specs=(vmem, vmem),
            scratch_shapes=scratch,
            compiler_params=pltpu.CompilerParams(
                collective_id=0, has_side_effects=True, vmem_limit_bytes=36 * 2**20
            ),
            name="mixer",
        )(
            *(
                pltpu.with_memory_space_constraint(array, pltpu.HBM)
                for array in (
                    inner, gate, proj.T, raw.T, conv_weight, conv_bias, step_bias, rate, skip
                )
            )
        )
        return pl.pallas_call(
            finale,
            out_shape=jax.ShapeDtypeStruct((rows, width), BF16),
            in_specs=[vmem, vmem, vmem],
            out_specs=hbm,
            scratch_shapes=[vm((rows, width), BF16), dma],
            compiler_params=pltpu.CompilerParams(vmem_limit_bytes=16 * 2**20),
            name="finale",
        )(gated, sumsq, gain.reshape(1, width))

    spec = P(("img", "seq"), None)
    return jax.shard_map(
        local,
        mesh=mesh,
        in_specs=(spec, spec, spec, spec, P(), P(), P(), P(), P(), P()),
        out_specs=spec,
        check_vma=False,
    )
```

```python
import functools

import jax
import jax.numpy as jnp
from jax import lax
from jax.experimental import pallas as pl
from jax.experimental.pallas import tpu as pltpu
from jax.sharding import PartitionSpec as P

MESH = pl.DeviceIdType.MESH
F32 = jnp.float32
BF16 = jnp.bfloat16
LANES = 128
HEAD = 64
GROUP = 8
NEAR = (6, 5, 7, 2, 4, 1, 3)
FAR = (4, 3, 5, 2, 6, 1, 7)
BAND = 32
EDGE = 16
HALO = 4


def split(v):
    high = v.astype(BF16).astype(F32)
    return jnp.concatenate([high, v - high], axis=1).astype(BF16)


def spreader(block, heads, rows):
    row = lax.broadcasted_iota(jnp.int32, (rows, LANES), 0)
    lane = lax.broadcasted_iota(jnp.int32, (rows, LANES), 1)
    row = jnp.where(row >= heads, row - heads, row)
    head = 2 * block + jnp.where(lane >= HEAD, 1, 0)
    return jnp.where(row == head, 1.0, 0.0).astype(BF16)


def dot(a, b):
    return jnp.dot(a, b, preferred_element_type=F32)


def silu(v):
    half = 0.5 * v
    return half + half * jnp.tanh(half)


def kernel(
    n, group, heads, kernel_taps,
    x_hbm, gate_hbm, proj_hbm, raw_hbm, cw_hbm, cb_hbm, sb_hbm, rate_hbm, skip_hbm,
    u, sumsq,
    xb, gb, xs, cf, cr, gf, gr, ef, er, gw, ext,
    proj_v, raw_v, cw_v, cb_v, sb_v, rate_v, skip_v,
    lhs, mf, mr, bt, cm,
    prev_v, next_v, tot_v, tots_v, totg_v, totr_v,
    send1, recv1, send2, recv2, send3, recv3,
    e_sem, x_sem, g_sem, s_sem, ready, h_send, h_recv,
    t1_send, t1_recv, t2_send, t2_recv, c1_send, c1_recv, c2_send, c2_recv, c3_send, c3_recv,
):
    rows = u.shape[1]
    blocks = u.shape[0]
    per = blocks // group
    groups = n // group
    states = bt.shape[1]
    me = lax.axis_index("seq")
    mem = lax.rem(me, group)
    grp = lax.div(me, group)
    base = me - mem

    def lanes(j):
        return pl.ds(pl.multiple_of(j * LANES, LANES), LANES)

    def pick(table, r):
        if isinstance(r, int):
            return table[r - 1]
        found = 0
        for k, value in enumerate(table):
            found = found + jnp.where(r == k + 1, value, 0)
        return found

    def offset(r, way):
        if group != 8:
            return lax.rem(mem + way * r + group, group)
        code = pick(NEAR, r)
        high, low = (divmod(code, 4)) if isinstance(code, int) else (lax.div(code, 4), lax.rem(code, 4))
        across = lax.rem(lax.div(mem, 4) + high, 2)
        return across * 4 + lax.rem(lax.rem(mem, 4) + way * low + 4, 4)

    def member(r):
        return offset(r, 1)

    def far(r):
        return lax.rem(grp + (pick(FAR, r) if groups == 8 else r), groups)

    def sweep(body, many):
        def turn(i, carry):
            for q in range(many):
                body(i * many + q)
            return carry

        lax.fori_loop(0, blocks // many, turn, 0)

    small = [
        (raw_hbm, raw_v), (sb_hbm, sb_v), (rate_hbm, rate_v), (proj_hbm, proj_v),
        (skip_hbm, skip_v), (cw_hbm, cw_v), (cb_hbm, cb_v),
    ]
    loads = [pltpu.make_async_copy(a, b, s_sem.at[i]) for i, (a, b) in enumerate(small)]
    bands = rows // BAND

    def x_copy(first, count, semaphore):
        band = pl.ds(first, count)
        return pltpu.make_async_copy(x_hbm.at[band], xb.at[band], semaphore)

    borders = [x_copy(0, EDGE, e_sem.at[0]), x_copy(rows - EDGE, EDGE, e_sem.at[1])]
    middle = x_copy(EDGE, rows - 2 * EDGE, x_sem)
    for copy in borders + loads + [middle]:
        copy.start()

    def g_copy(i):
        band = pl.ds(i * BAND, BAND)
        return pltpu.make_async_copy(gate_hbm.at[band], gb.at[band], g_sem)

    barrier = pltpu.get_barrier_semaphore()
    after = lax.rem(me + 1, n)
    before = lax.rem(me + n - 1, n)
    beside = (lax.rem(me + group, n), lax.rem(me + n - group, n))

    def signal(semaphore, peer):
        pl.semaphore_signal(semaphore, inc=1, device_id={"seq": peer}, device_id_type=MESH)

    for peer in (after, before) + beside:
        signal(barrier, peer)
    for r in range(1, group):
        signal(barrier, base + member(r))

    for i in range(bands):
        g_copy(i).start()

    pl.semaphore_wait(barrier, 4 + (group - 1))
    for copy in borders:
        copy.wait()
    halo = [
        pltpu.make_async_remote_copy(
            src_ref=xb.at[pl.ds(rows - HALO, HALO)], dst_ref=prev_v,
            send_sem=h_send.at[0], recv_sem=h_recv.at[0],
            device_id={"seq": after}, device_id_type=MESH,
        ),
        pltpu.make_async_remote_copy(
            src_ref=xb.at[pl.ds(0, HALO)], dst_ref=next_v,
            send_sem=h_send.at[1], recv_sem=h_recv.at[1],
            device_id={"seq": before}, device_id_type=MESH,
        ),
    ]
    for copy in halo:
        copy.start()
    rounds = groups // 2 - 1

    def relay(k):
        if 0 < k <= rounds:
            pl.semaphore_wait(ready.at[k - 1], 2)
        if k < rounds:
            for peer in beside:
                signal(ready.at[k], peer)

    relay(0)
    first_t = lax.broadcasted_iota(jnp.int32, (rows, rows), 0)
    second_t = lax.broadcasted_iota(jnp.int32, (rows, rows), 1)
    masks = (first_t >= second_t, first_t <= second_t)
    for copy in loads[:5]:
        copy.wait()

    lasts = (rows - 1, 0)
    raw = raw_v[...].astype(F32)
    params = jnp.concatenate(
        [
            jnp.concatenate([sb_v[...], rate_v[...], jnp.zeros((4, heads), F32)], axis=0),
            jnp.zeros((8, LANES - heads), F32),
        ],
        axis=1,
    ).T
    zeros = jnp.zeros((16 - 4, heads), F32)
    grow, decay, total, skips = [], [], [], []
    for d in range(2):
        v = raw[d * heads : (d + 1) * heads] + params[:heads, d : d + 1]
        step = jnp.maximum(v, 0.0) + jnp.log1p(jnp.exp(-jnp.abs(v)))
        cumul = jnp.dot(
            -params[:heads, 2 + d : 3 + d] * step,
            jnp.where(masks[1 - d], 1.0, 0.0),
            precision=lax.Precision.HIGHEST,
            preferred_element_type=F32,
        )
        grow.append((jnp.exp(-cumul) * step).T)
        decay.append(jnp.exp(cumul).T)
        total.append(decay[d][lasts[d] : lasts[d] + 1, :])
        skips.append(skip_v[d : d + 1, :])
        first = 2 * d * states
        write_t = proj_v[first : first + states, :]
        read = proj_v[first + states : first + 2 * states, :].astype(F32).T.astype(BF16)
        bt[d] = write_t
        cm[d] = read
        scores = jnp.where(masks[d], dot(read, write_t), 0.0).astype(BF16)
        (mf, mr)[d][...] = scores
    lhs[...] = split(jnp.concatenate(decay + grow + total + skips + [zeros], axis=0))
    tot_v[...] = jnp.concatenate(
        [
            jnp.concatenate(total, axis=0),
            jnp.zeros((2, LANES - heads), F32),
        ],
        axis=1,
    )

    def near_copy(src, dst, ss, rs, r):
        return pltpu.make_async_remote_copy(
            src_ref=src, dst_ref=dst, send_sem=ss, recv_sem=rs,
            device_id={"seq": base + member(r)}, device_id_type=MESH,
        )

    def far_copy(src, dst, ss, rs, r):
        return pltpu.make_async_remote_copy(
            src_ref=src, dst_ref=dst, send_sem=ss, recv_sem=rs,
            device_id={"seq": far(r) * group + mem}, device_id_type=MESH,
        )

    def t1(r):
        return near_copy(tot_v, tots_v.at[mem], t1_send, t1_recv, r)

    def t2(r):
        return far_copy(totg_v, totr_v.at[grp], t2_send, t2_recv, r)

    def c1(r):
        return near_copy(send1.at[member(r)], recv1.at[mem], c1_send, c1_recv, r)

    def c2(r, b):
        ahead = jnp.where(far(r) > grp, 0, 1)
        return far_copy(
            send2.at[ahead, b], recv2.at[b, grp], c2_send.at[b], c2_recv.at[b], r
        )

    def c3(r, b):
        return near_copy(
            send3.at[b, member(r)], recv3.at[b, mem], c3_send.at[b], c3_recv.at[b], r
        )

    near_all, far_all = pl.ds(0, group - 1), pl.ds(0, groups - 1)
    t1_all = near_copy(tots_v.at[near_all], tots_v.at[near_all], t1_send, t1_recv, 1)
    t2_all = far_copy(totr_v.at[far_all], totr_v.at[far_all], t2_send, t2_recv, 1)
    c1_all = near_copy(send1.at[near_all], recv1.at[near_all], c1_send, c1_recv, 1)

    def c2_all(b):
        whole = recv2.at[b, far_all]
        return far_copy(whole, whole, c2_send.at[b], c2_recv.at[b], 1)

    def c3_all(b):
        return near_copy(
            send3.at[b, near_all], recv3.at[b, near_all], c3_send.at[b], c3_recv.at[b], 1
        )


    def loop(first, last, action):
        def body(r, carry):
            action(r)
            return carry

        lax.fori_loop(first, last, body, 0)

    for r in range(1, group):
        t1(r).start()
    tots_v[mem] = tot_v[...]

    def growth(j):
        wide = dot(lhs[pl.ds(2 * rows, 2 * rows + 16), :], spreader(j, heads, 2 * heads))
        gw[0, j] = wide[:rows]
        gw[1, j] = wide[rows : 2 * rows]
        ext[j] = wide[2 * rows : 2 * rows + 8]

    sweep(growth, 12)
    relay(1)
    for copy in loads[5:]:
        copy.wait()
    middle.wait()
    for copy in halo:
        copy.wait()

    has_before = jnp.where(me > 0, 1.0, 0.0)
    has_after = jnp.where(me < n - 1, 1.0, 0.0)

    def conv(owner):
        for b in range(per):
            j = owner * per + b
            xs[j, pl.ds(8 - HALO, HALO), :] = prev_v[:, lanes(j)].astype(F32) * has_before
            xs[j, pl.ds(8 + rows, HALO), :] = next_v[:, lanes(j)].astype(F32) * has_after
            xs[j, pl.ds(8, rows), :] = xb[:, lanes(j)].astype(F32)
        for b in range(per):
            j = owner * per + b
            for d in range(2):
                acc = 0.5 * cb_v[d : d + 1, lanes(j)]
                for k in range(kernel_taps):
                    shift = -k if d == 0 else k
                    tap = 0.5 * cw_v[d, k : k + 1, lanes(j)]
                    acc = acc + tap * xs[j, pl.ds(8 + shift, rows), :]
                conved = (acc + acc * jnp.tanh(acc)).astype(BF16)
                (cf, cr)[d][j] = conved
                (gf, gr)[d][j] = (gw[d, j] * conved.astype(F32)).astype(BF16)

    def finish(owner, buffer):
        results = []
        for b in range(per):
            j = owner * per + b
            for d in range(2):
                end = dot(bt[d], (gf, gr)[d][j]) * ext[j, pl.ds(d, 1), :]
                results.append((b, d, end.astype(BF16)))
        for b, d, end in results:
            buffer[owner, b, pl.ds(d * states, states), :] = end

    conv(member(1))

    def ends(r):
        finish(member(r), send1)
        conv(member(r + 1))
        c1(r).start()

    loop(1, group, ends)
    finish(mem, recv1)
    relay(2)

    t1_all.wait()
    product = tots_v[0]
    for m in range(1, group):
        product = product * tots_v[m]
    totg_v[...] = product
    totr_v[grp] = product
    pltpu.make_async_copy(gate_hbm, gb, g_sem).wait()

    def inner(j):
        wide = dot(lhs[pl.ds(0, 2 * rows), :], spreader(j, heads, 2 * heads))
        gate = silu(gb[:, lanes(j)].astype(F32))
        far_f, far_r = wide[:rows] * gate, wide[rows:] * gate
        ef[j] = far_f
        er[j] = far_r
        direct = (
            ext[j, pl.ds(2, 1), :] * cf[j].astype(F32) + ext[j, pl.ds(3, 1), :] * cr[j].astype(F32)
        )
        u[j] = direct * gate + far_f * dot(mf[...], gf[j]) + far_r * dot(mr[...], gr[j])

    sweep(inner, 4)
    relay(3)
    for r in range(1, groups):
        t2(r).start()

    c1_all.wait_recv()

    def spread(values, b):
        flat = values[...].reshape(-1, LANES)
        high = flat.astype(BF16)
        low = (flat - high.astype(F32)).astype(BF16)
        ones = spreader(mem * per + b, LANES, LANES)
        return dot(high, ones) + dot(low, ones)

    near_t = [spread(tots_v, b) for b in range(per)]

    def part(ref, m, b, d):
        return ref[m, b, pl.ds(d * states, states), :].astype(F32)

    for b in range(per):
        run_f = jnp.zeros((states, LANES), F32)
        run_r = jnp.zeros((states, LANES), F32)
        for m in range(group):
            run_f = run_f * near_t[b][2 * m : 2 * m + 1] + part(recv1, m, b, 0)
            k = group - 1 - m
            run_r = run_r * near_t[b][2 * k + 1 : 2 * k + 2] + part(recv1, k, b, 1)
        send2[0, b] = run_f.astype(BF16)
        send2[1, b] = run_r.astype(BF16)
        for r in range(1, groups):
            c2(r, b).start()
    t2_all.wait()
    far_t = [spread(totr_v, b) for b in range(per)]
    for b in range(per):
        recv2[b, grp] = send2[0, b]

    for b in range(per):
        c2_all(b).wait_recv()
        run_f = jnp.zeros((states, LANES), F32)
        run_r = jnp.zeros((states, LANES), F32)
        for g in range(groups):
            new = run_f * far_t[b][2 * g : 2 * g + 1] + recv2[b, g].astype(F32)
            run_f = jnp.where(g < grp, new, run_f)
            k = groups - 1 - g
            new = run_r * far_t[b][2 * k + 1 : 2 * k + 2] + recv2[b, k].astype(F32)
            run_r = jnp.where(k > grp, new, run_r)
        for m in range(group):
            send3[b, m, pl.ds(0, states), :] = run_f.astype(BF16)
            run_f = run_f * near_t[b][2 * m : 2 * m + 1] + part(recv1, m, b, 0)
            k = group - 1 - m
            send3[b, k, pl.ds(states, states), :] = run_r.astype(BF16)
            run_r = run_r * near_t[b][2 * k + 1 : 2 * k + 2] + part(recv1, k, b, 1)
        for r in range(1, group):
            c3(r, b).start()
        recv3[b, mem] = send3[b, mem]

    sumsq[...] = jnp.zeros_like(sumsq)
    many = min(4, group)
    for b in range(per):
        c3_all(b).wait_recv()

        def outer(i, carry):
            squares = jnp.zeros((rows, LANES), F32)
            for q in range(many):
                owner = i * many + q
                j = owner * per + b
                gated = (
                    u[j]
                    + ef[j] * dot(cm[0], recv3[b, owner, pl.ds(0, states), :])
                    + er[j] * dot(cm[1], recv3[b, owner, pl.ds(states, states), :])
                )
                u[j] = gated
                squares = squares + gated * gated
            sumsq[...] += squares
            return carry

        lax.fori_loop(0, group // many, outer, 0)

    c1_all.wait_send()
    for b in range(per):
        c2_all(b).wait_send()
        c3_all(b).wait_send()


def finale(u, sumsq, gain, out_hbm, ob, o_sem):
    blocks, rows, _ = u.shape
    mean = jnp.sum(sumsq[...], axis=1, keepdims=True) * (1.0 / (blocks * LANES))
    scale = lax.rsqrt(mean + 1e-05)
    for i in range(rows // 16):
        part = slice(i * 16, (i + 1) * 16)
        for j in range(blocks):
            lanes = slice(j * LANES, (j + 1) * LANES)
            ob[part, lanes] = (u[j, part] * scale[part] * gain[:, lanes]).astype(BF16)
        band = pl.ds(i * 16, 16)
        pltpu.make_async_copy(ob.at[band], out_hbm.at[band], o_sem).start()
    pltpu.make_async_copy(ob, out_hbm, o_sem).wait()


def solution(mesh, group=GROUP):
    n = mesh.shape["seq"]

    def local(inner, gate, proj, raw, conv_weight, conv_bias, step_bias, rate, skip, gain):
        rows, width = inner.shape
        heads = width // HEAD
        blocks = width // LANES
        per = blocks // group
        groups = n // group
        states = proj.shape[1] // 4
        taps = conv_weight.shape[1]
        dma = pltpu.SemaphoreType.DMA
        vm = pltpu.VMEM
        wide16 = vm((blocks, rows, LANES), BF16)
        wide32 = vm((blocks, rows, LANES), F32)
        scratch = [
            vm((rows, width), BF16),
            vm((rows, width), BF16),
            vm((blocks, rows + 16, LANES), F32),
            wide16,
            wide16,
            wide16,
            wide16,
            wide32,
            wide32,
            vm((2, blocks, rows, LANES), F32),
            vm((blocks, 8, LANES), F32),
            vm(proj.shape[::-1], BF16),
            vm(raw.shape[::-1], BF16),
            vm(conv_weight.shape, F32),
            vm(conv_bias.shape, F32),
            vm(step_bias.shape, F32),
            vm(rate.shape, F32),
            vm(skip.shape, F32),
            vm((4 * rows + 16, 2 * heads), BF16),
            vm((rows, rows), BF16),
            vm((rows, rows), BF16),
            vm((2, states, rows), BF16),
            vm((2, rows, states), BF16),
            vm((HALO, width), BF16),
            vm((HALO, width), BF16),
            vm((2, LANES), F32),
            vm((group, 2, LANES), F32),
            vm((2, LANES), F32),
            vm((groups, 2, LANES), F32),
            vm((group, per, 2 * states, LANES), BF16),
            vm((group, per, 2 * states, LANES), BF16),
            vm((2, per, states, LANES), BF16),
            vm((per, groups, states, LANES), BF16),
            vm((per, group, 2 * states, LANES), BF16),
            vm((per, group, 2 * states, LANES), BF16),
            dma((2,)),
            dma,
            dma,
            dma((7,)),
            pltpu.SemaphoreType.REGULAR((max(1, groups // 2 - 1),)),
            dma((2,)),
            dma((2,)),
        ]
        scratch += [dma] * 6 + [dma((per,))] * 4
        vmem = pl.BlockSpec(memory_space=pltpu.VMEM)
        hbm = pl.BlockSpec(memory_space=pl.ANY)
        gated, sumsq = pl.pallas_call(
            functools.partial(kernel, n, group, heads, taps),
            out_shape=(
                jax.ShapeDtypeStruct((blocks, rows, LANES), F32),
                jax.ShapeDtypeStruct((rows, LANES), F32),
            ),
            in_specs=[hbm] * 9,
            out_specs=(vmem, vmem),
            scratch_shapes=scratch,
            compiler_params=pltpu.CompilerParams(
                collective_id=0, has_side_effects=True, vmem_limit_bytes=36 * 2**20
            ),
            name="mixer",
        )(
            *(
                pltpu.with_memory_space_constraint(array, pltpu.HBM)
                for array in (
                    inner, gate, proj.T, raw.T, conv_weight, conv_bias, step_bias, rate, skip
                )
            )
        )
        return pl.pallas_call(
            finale,
            out_shape=jax.ShapeDtypeStruct((rows, width), BF16),
            in_specs=[vmem, vmem, vmem],
            out_specs=hbm,
            scratch_shapes=[vm((rows, width), BF16), dma],
            compiler_params=pltpu.CompilerParams(vmem_limit_bytes=16 * 2**20),
            name="finale",
        )(gated, sumsq, gain.reshape(1, width))

    spec = P(("img", "seq"), None)
    return jax.shard_map(
        local,
        mesh=mesh,
        in_specs=(spec, spec, spec, spec, P(), P(), P(), P(), P(), P()),
        out_specs=spec,
        check_vma=False,
    )
```

```python
import functools

import jax
import jax.numpy as jnp
from jax import lax
from jax.experimental import pallas as pl
from jax.experimental.pallas import tpu as pltpu
from jax.sharding import PartitionSpec as P

MESH = pl.DeviceIdType.MESH
F32 = jnp.float32
BF16 = jnp.bfloat16
LANES = 128
HEAD = 64
GROUP = 8
NEAR = (6, 5, 7, 2, 4, 1, 3)
FAR = (4, 3, 5, 2, 6, 1, 7)
BAND = 32
EDGE = 16
HALO = 4


def split(v):
    high = v.astype(BF16).astype(F32)
    return jnp.concatenate([high, v - high], axis=1).astype(BF16)


def spreader(block, heads, rows):
    row = lax.broadcasted_iota(jnp.int32, (rows, LANES), 0)
    lane = lax.broadcasted_iota(jnp.int32, (rows, LANES), 1)
    row = jnp.where(row >= heads, row - heads, row)
    head = 2 * block + jnp.where(lane >= HEAD, 1, 0)
    return jnp.where(row == head, 1.0, 0.0).astype(BF16)


def dot(a, b):
    return jnp.dot(a, b, preferred_element_type=F32)


def silu(v):
    half = 0.5 * v
    return half + half * jnp.tanh(half)


def kernel(
    n, group, heads, kernel_taps,
    x_hbm, gate_hbm, proj_hbm, raw_hbm, cw_hbm, cb_hbm, sb_hbm, rate_hbm, skip_hbm,
    u, sumsq,
    xb, gb, xs, cf, cr, gf, gr, ef, er, gw, ext,
    proj_v, raw_v, cw_v, cb_v, sb_v, rate_v, skip_v,
    lhs, mf, mr, bt, cm,
    prev_v, next_v, tot_v, tots_v, totg_v, totr_v,
    send1, recv1, send2, recv2, send3, recv3,
    e_sem, x_sem, g_sem, s_sem, ready, h_send, h_recv,
    t1_send, t1_recv, t2_send, t2_recv, c1_send, c1_recv, c2_send, c2_recv, c3_send, c3_recv,
):
    rows = u.shape[1]
    blocks = u.shape[0]
    per = blocks // group
    groups = n // group
    states = bt.shape[1]
    me = lax.axis_index("seq")
    mem = lax.rem(me, group)
    grp = lax.div(me, group)
    base = me - mem

    def lanes(j):
        return pl.ds(pl.multiple_of(j * LANES, LANES), LANES)

    def pick(table, r):
        if isinstance(r, int):
            return table[r - 1]
        found = 0
        for k, value in enumerate(table):
            found = found + jnp.where(r == k + 1, value, 0)
        return found

    def offset(r, way):
        if group != 8:
            return lax.rem(mem + way * r + group, group)
        code = pick(NEAR, r)
        high, low = (divmod(code, 4)) if isinstance(code, int) else (lax.div(code, 4), lax.rem(code, 4))
        across = lax.rem(lax.div(mem, 4) + high, 2)
        return across * 4 + lax.rem(lax.rem(mem, 4) + way * low + 4, 4)

    def member(r):
        return offset(r, 1)

    def far(r):
        return lax.rem(grp + (pick(FAR, r) if groups == 8 else r), groups)

    def sweep(body, many):
        def turn(i, carry):
            for q in range(many):
                body(i * many + q)
            return carry

        lax.fori_loop(0, blocks // many, turn, 0)

    barrier = pltpu.get_barrier_semaphore()
    after = lax.rem(me + 1, n)
    before = lax.rem(me + n - 1, n)
    beside = (lax.rem(me + group, n), lax.rem(me + n - group, n))

    def signal(semaphore, peer):
        pl.semaphore_signal(semaphore, inc=1, device_id={"seq": peer}, device_id_type=MESH)

    for peer in (after, before) + beside:
        signal(barrier, peer)
    for r in range(1, group):
        signal(barrier, base + member(r))

    small = [
        (raw_hbm, raw_v), (sb_hbm, sb_v), (rate_hbm, rate_v), (proj_hbm, proj_v),
        (skip_hbm, skip_v), (cw_hbm, cw_v), (cb_hbm, cb_v),
    ]
    loads = [pltpu.make_async_copy(a, b, s_sem.at[i]) for i, (a, b) in enumerate(small)]
    bands = rows // BAND

    def x_copy(first, count, semaphore):
        band = pl.ds(first, count)
        return pltpu.make_async_copy(x_hbm.at[band], xb.at[band], semaphore)

    borders = [x_copy(0, EDGE, e_sem.at[0]), x_copy(rows - EDGE, EDGE, e_sem.at[1])]
    middle = x_copy(EDGE, rows - 2 * EDGE, x_sem)
    for copy in borders + loads + [middle]:
        copy.start()

    def g_copy(i):
        band = pl.ds(i * BAND, BAND)
        return pltpu.make_async_copy(gate_hbm.at[band], gb.at[band], g_sem)

    for i in range(bands):
        g_copy(i).start()

    pl.semaphore_wait(barrier, 4 + (group - 1))
    for copy in borders:
        copy.wait()
    halo = [
        pltpu.make_async_remote_copy(
            src_ref=xb.at[pl.ds(rows - HALO, HALO)], dst_ref=prev_v,
            send_sem=h_send.at[0], recv_sem=h_recv.at[0],
            device_id={"seq": after}, device_id_type=MESH,
        ),
        pltpu.make_async_remote_copy(
            src_ref=xb.at[pl.ds(0, HALO)], dst_ref=next_v,
            send_sem=h_send.at[1], recv_sem=h_recv.at[1],
            device_id={"seq": before}, device_id_type=MESH,
        ),
    ]
    not_last, not_first = me < n - 1, me > 0

    @pl.when(not_last)
    def _():
        halo[0].start()

    @pl.when(not_first)
    def _():
        halo[1].start()

    @pl.when(me == 0)
    def _():
        prev_v[...] = jnp.zeros_like(prev_v)

    @pl.when(me == n - 1)
    def _():
        next_v[...] = jnp.zeros_like(next_v)

    rounds = groups // 2 - 1

    def relay(k):
        if 0 < k <= rounds:
            pl.semaphore_wait(ready.at[k - 1], 2)
        if k < rounds:
            for peer in beside:
                signal(ready.at[k], peer)

    relay(0)
    first_t = lax.broadcasted_iota(jnp.int32, (rows, rows), 0)
    second_t = lax.broadcasted_iota(jnp.int32, (rows, rows), 1)
    masks = (first_t >= second_t, first_t <= second_t)
    for copy in loads[:5]:
        copy.wait()

    lasts = (rows - 1, 0)
    raw = raw_v[...].astype(F32)
    params = jnp.concatenate(
        [
            jnp.concatenate([sb_v[...], rate_v[...], jnp.zeros((4, heads), F32)], axis=0),
            jnp.zeros((8, LANES - heads), F32),
        ],
        axis=1,
    ).T
    zeros = jnp.zeros((16 - 4, heads), F32)
    grow, decay, total, skips = [], [], [], []
    for d in range(2):
        v = raw[d * heads : (d + 1) * heads] + params[:heads, d : d + 1]
        step = jnp.maximum(v, 0.0) + jnp.log1p(jnp.exp(-jnp.abs(v)))
        cumul = jnp.dot(
            -params[:heads, 2 + d : 3 + d] * step,
            jnp.where(masks[1 - d], 1.0, 0.0),
            precision=lax.Precision.HIGHEST,
            preferred_element_type=F32,
        )
        grow.append((jnp.exp(-cumul) * step).T)
        decay.append(jnp.exp(cumul).T)
        total.append(decay[d][lasts[d] : lasts[d] + 1, :])
        skips.append(skip_v[d : d + 1, :])
        first = 2 * d * states
        write_t = proj_v[first : first + states, :]
        read = proj_v[first + states : first + 2 * states, :].astype(F32).T.astype(BF16)
        bt[d] = write_t
        cm[d] = read
        scores = jnp.where(masks[d], dot(read, write_t), 0.0).astype(BF16)
        (mf, mr)[d][...] = scores
    lhs[...] = split(jnp.concatenate(decay + grow + total + skips + [zeros], axis=0))
    tot_v[...] = jnp.concatenate(
        [
            jnp.concatenate(total, axis=0),
            jnp.zeros((2, LANES - heads), F32),
        ],
        axis=1,
    )

    def near_copy(src, dst, ss, rs, r):
        return pltpu.make_async_remote_copy(
            src_ref=src, dst_ref=dst, send_sem=ss, recv_sem=rs,
            device_id={"seq": base + member(r)}, device_id_type=MESH,
        )

    def far_copy(src, dst, ss, rs, r):
        return pltpu.make_async_remote_copy(
            src_ref=src, dst_ref=dst, send_sem=ss, recv_sem=rs,
            device_id={"seq": far(r) * group + mem}, device_id_type=MESH,
        )

    def t1(r):
        return near_copy(tot_v, tots_v.at[mem], t1_send, t1_recv, r)

    def t2(r):
        return far_copy(totg_v, totr_v.at[grp], t2_send, t2_recv, r)

    def c1(r):
        return near_copy(send1.at[member(r)], recv1.at[mem], c1_send, c1_recv, r)

    def c2(r, b):
        ahead = jnp.where(far(r) > grp, 0, 1)
        return far_copy(
            send2.at[ahead, b], recv2.at[b, grp], c2_send.at[b], c2_recv.at[b], r
        )

    def c3(r, b):
        return near_copy(
            send3.at[b, member(r)], recv3.at[b, mem], c3_send.at[b], c3_recv.at[b], r
        )

    near_all, far_all = pl.ds(0, group - 1), pl.ds(0, groups - 1)
    t1_all = near_copy(tots_v.at[near_all], tots_v.at[near_all], t1_send, t1_recv, 1)
    t2_all = far_copy(totr_v.at[far_all], totr_v.at[far_all], t2_send, t2_recv, 1)
    c1_all = near_copy(send1.at[near_all], recv1.at[near_all], c1_send, c1_recv, 1)

    def c2_all(b):
        whole = recv2.at[b, far_all]
        return far_copy(whole, whole, c2_send.at[b], c2_recv.at[b], 1)

    def c3_all(b):
        return near_copy(
            send3.at[b, near_all], recv3.at[b, near_all], c3_send.at[b], c3_recv.at[b], 1
        )


    def loop(first, last, action):
        def body(r, carry):
            action(r)
            return carry

        lax.fori_loop(first, last, body, 0)

    for r in range(1, group):
        t1(r).start()
    tots_v[mem] = tot_v[...]

    def growth(j):
        wide = dot(lhs[pl.ds(2 * rows, 2 * rows + 16), :], spreader(j, heads, 2 * heads))
        gw[0, j] = wide[:rows]
        gw[1, j] = wide[rows : 2 * rows]
        ext[j] = wide[2 * rows : 2 * rows + 8]

    sweep(growth, 12)
    relay(1)
    for copy in loads[5:]:
        copy.wait()
    middle.wait()

    @pl.when(not_last)
    def _():
        halo[0].wait_send()
        halo[1].wait_recv()

    @pl.when(not_first)
    def _():
        halo[1].wait_send()
        halo[0].wait_recv()

    def conv(owner):
        for b in range(per):
            j = owner * per + b
            xs[j, pl.ds(8 - HALO, HALO), :] = prev_v[:, lanes(j)].astype(F32)
            xs[j, pl.ds(8 + rows, HALO), :] = next_v[:, lanes(j)].astype(F32)
            xs[j, pl.ds(8, rows), :] = xb[:, lanes(j)].astype(F32)
        for b in range(per):
            j = owner * per + b
            for d in range(2):
                acc = 0.5 * cb_v[d : d + 1, lanes(j)]
                for k in range(kernel_taps):
                    shift = -k if d == 0 else k
                    tap = 0.5 * cw_v[d, k : k + 1, lanes(j)]
                    acc = acc + tap * xs[j, pl.ds(8 + shift, rows), :]
                conved = (acc + acc * jnp.tanh(acc)).astype(BF16)
                (cf, cr)[d][j] = conved
                (gf, gr)[d][j] = (gw[d, j] * conved.astype(F32)).astype(BF16)

    def finish(owner, buffer):
        results = []
        for b in range(per):
            j = owner * per + b
            for d in range(2):
                end = dot(bt[d], (gf, gr)[d][j]) * ext[j, pl.ds(d, 1), :]
                results.append((b, d, end.astype(BF16)))
        for b, d, end in results:
            buffer[owner, b, pl.ds(d * states, states), :] = end

    conv(member(1))

    def ends(r):
        finish(member(r), send1)
        conv(member(r + 1))
        c1(r).start()

    loop(1, group - 1, ends)
    finish(member(group - 1), send1)
    c1(group - 1).start()
    conv(mem)
    finish(mem, recv1)
    relay(2)

    t1_all.wait()
    product = tots_v[0]
    for m in range(1, group):
        product = product * tots_v[m]
    totg_v[...] = product
    totr_v[grp] = product
    pltpu.make_async_copy(gate_hbm, gb, g_sem).wait()

    def inner(j):
        wide = dot(lhs[pl.ds(0, 2 * rows), :], spreader(j, heads, 2 * heads))
        gate = silu(gb[:, lanes(j)].astype(F32))
        far_f, far_r = wide[:rows] * gate, wide[rows:] * gate
        ef[j] = far_f
        er[j] = far_r
        direct = (
            ext[j, pl.ds(2, 1), :] * cf[j].astype(F32) + ext[j, pl.ds(3, 1), :] * cr[j].astype(F32)
        )
        u[j] = direct * gate + far_f * dot(mf[...], gf[j]) + far_r * dot(mr[...], gr[j])

    sweep(inner, 4)
    relay(3)
    for r in range(1, groups):
        t2(r).start()

    c1_all.wait_recv()

    def spread(values, b):
        flat = values[...].reshape(-1, LANES)
        high = flat.astype(BF16)
        low = (flat - high.astype(F32)).astype(BF16)
        ones = spreader(mem * per + b, LANES, LANES)
        return dot(high, ones) + dot(low, ones)

    near_t = [spread(tots_v, b) for b in range(per)]

    def part(ref, m, b, d):
        return ref[m, b, pl.ds(d * states, states), :].astype(F32)

    for b in range(per):
        run_f = jnp.zeros((states, LANES), F32)
        run_r = jnp.zeros((states, LANES), F32)
        for m in range(group):
            run_f = run_f * near_t[b][2 * m : 2 * m + 1] + part(recv1, m, b, 0)
            k = group - 1 - m
            run_r = run_r * near_t[b][2 * k + 1 : 2 * k + 2] + part(recv1, k, b, 1)
        send2[0, b] = run_f.astype(BF16)
        send2[1, b] = run_r.astype(BF16)
        for r in range(1, groups):
            c2(r, b).start()
    t2_all.wait()
    far_t = [spread(totr_v, b) for b in range(per)]
    for b in range(per):
        recv2[b, grp] = send2[0, b]

    for b in range(per):
        c2_all(b).wait_recv()
        run_f = jnp.zeros((states, LANES), F32)
        run_r = jnp.zeros((states, LANES), F32)
        for g in range(groups):
            new = run_f * far_t[b][2 * g : 2 * g + 1] + recv2[b, g].astype(F32)
            run_f = jnp.where(g < grp, new, run_f)
            k = groups - 1 - g
            new = run_r * far_t[b][2 * k + 1 : 2 * k + 2] + recv2[b, k].astype(F32)
            run_r = jnp.where(k > grp, new, run_r)
        for m in range(group):
            send3[b, m, pl.ds(0, states), :] = run_f.astype(BF16)
            run_f = run_f * near_t[b][2 * m : 2 * m + 1] + part(recv1, m, b, 0)
            k = group - 1 - m
            send3[b, k, pl.ds(states, states), :] = run_r.astype(BF16)
            run_r = run_r * near_t[b][2 * k + 1 : 2 * k + 2] + part(recv1, k, b, 1)
        for r in range(1, group):
            c3(r, b).start()
        recv3[b, mem] = send3[b, mem]

    sumsq[...] = jnp.zeros_like(sumsq)
    many = min(8, group)
    for b in range(per):
        c3_all(b).wait_recv()

        def outer(i, carry):
            squares = jnp.zeros((rows, LANES), F32)
            for q in range(many):
                owner = i * many + q
                j = owner * per + b
                gated = (
                    u[j]
                    + ef[j] * dot(cm[0], recv3[b, owner, pl.ds(0, states), :])
                    + er[j] * dot(cm[1], recv3[b, owner, pl.ds(states, states), :])
                )
                u[j] = gated
                squares = squares + gated * gated
            sumsq[...] += squares
            return carry

        lax.fori_loop(0, group // many, outer, 0)

    c1_all.wait_send()
    for b in range(per):
        c2_all(b).wait_send()
        c3_all(b).wait_send()


def finale(u, sumsq, gain, out_hbm, ob, o_sem):
    blocks, rows, _ = u.shape
    mean = jnp.sum(sumsq[...], axis=1, keepdims=True) * (1.0 / (blocks * LANES))
    scale = lax.rsqrt(mean + 1e-05)
    for i in range(rows // 16):
        part = slice(i * 16, (i + 1) * 16)
        for j in range(blocks):
            lanes = slice(j * LANES, (j + 1) * LANES)
            ob[part, lanes] = (u[j, part] * scale[part] * gain[:, lanes]).astype(BF16)
        band = pl.ds(i * 16, 16)
        pltpu.make_async_copy(ob.at[band], out_hbm.at[band], o_sem).start()
    pltpu.make_async_copy(ob, out_hbm, o_sem).wait()


def solution(mesh, group=GROUP):
    n = mesh.shape["seq"]

    def local(inner, gate, proj, raw, conv_weight, conv_bias, step_bias, rate, skip, gain):
        rows, width = inner.shape
        heads = width // HEAD
        blocks = width // LANES
        per = blocks // group
        groups = n // group
        states = proj.shape[1] // 4
        taps = conv_weight.shape[1]
        dma = pltpu.SemaphoreType.DMA
        vm = pltpu.VMEM
        wide16 = vm((blocks, rows, LANES), BF16)
        wide32 = vm((blocks, rows, LANES), F32)
        scratch = [
            vm((rows, width), BF16),
            vm((rows, width), BF16),
            vm((blocks, rows + 16, LANES), F32),
            wide16,
            wide16,
            wide16,
            wide16,
            wide32,
            wide32,
            vm((2, blocks, rows, LANES), F32),
            vm((blocks, 8, LANES), F32),
            vm(proj.shape[::-1], BF16),
            vm(raw.shape[::-1], BF16),
            vm(conv_weight.shape, F32),
            vm(conv_bias.shape, F32),
            vm(step_bias.shape, F32),
            vm(rate.shape, F32),
            vm(skip.shape, F32),
            vm((4 * rows + 16, 2 * heads), BF16),
            vm((rows, rows), BF16),
            vm((rows, rows), BF16),
            vm((2, states, rows), BF16),
            vm((2, rows, states), BF16),
            vm((HALO, width), BF16),
            vm((HALO, width), BF16),
            vm((2, LANES), F32),
            vm((group, 2, LANES), F32),
            vm((2, LANES), F32),
            vm((groups, 2, LANES), F32),
            vm((group, per, 2 * states, LANES), BF16),
            vm((group, per, 2 * states, LANES), BF16),
            vm((2, per, states, LANES), BF16),
            vm((per, groups, states, LANES), BF16),
            vm((per, group, 2 * states, LANES), BF16),
            vm((per, group, 2 * states, LANES), BF16),
            dma((2,)),
            dma,
            dma,
            dma((7,)),
            pltpu.SemaphoreType.REGULAR((max(1, groups // 2 - 1),)),
            dma((2,)),
            dma((2,)),
        ]
        scratch += [dma] * 6 + [dma((per,))] * 4
        vmem = pl.BlockSpec(memory_space=pltpu.VMEM)
        hbm = pl.BlockSpec(memory_space=pl.ANY)
        gated, sumsq = pl.pallas_call(
            functools.partial(kernel, n, group, heads, taps),
            out_shape=(
                jax.ShapeDtypeStruct((blocks, rows, LANES), F32),
                jax.ShapeDtypeStruct((rows, LANES), F32),
            ),
            in_specs=[hbm] * 9,
            out_specs=(vmem, vmem),
            scratch_shapes=scratch,
            compiler_params=pltpu.CompilerParams(
                collective_id=0, has_side_effects=True, vmem_limit_bytes=36 * 2**20
            ),
            name="mixer",
        )(
            *(
                pltpu.with_memory_space_constraint(array, pltpu.HBM)
                for array in (
                    inner, gate, proj.T, raw.T, conv_weight, conv_bias, step_bias, rate, skip
                )
            )
        )
        return pl.pallas_call(
            finale,
            out_shape=jax.ShapeDtypeStruct((rows, width), BF16),
            in_specs=[vmem, vmem, vmem],
            out_specs=hbm,
            scratch_shapes=[vm((rows, width), BF16), dma],
            compiler_params=pltpu.CompilerParams(vmem_limit_bytes=16 * 2**20),
            name="finale",
        )(gated, sumsq, gain.reshape(1, width))

    spec = P(("img", "seq"), None)
    return jax.shard_map(
        local,
        mesh=mesh,
        in_specs=(spec, spec, spec, spec, P(), P(), P(), P(), P(), P()),
        out_specs=spec,
        check_vma=False,
    )
```

```python
import functools

import jax
import jax.numpy as jnp
from jax import lax
from jax.experimental import pallas as pl
from jax.experimental.pallas import tpu as pltpu
from jax.sharding import PartitionSpec as P

MESH = pl.DeviceIdType.MESH
F32 = jnp.float32
BF16 = jnp.bfloat16
LANES = 128
HEAD = 64
GROUP = 8
NEAR = (6, 5, 7, 2, 4, 1, 3)
FAR = (4, 3, 5, 2, 6, 1, 7)
BAND = 32
EDGE = 16
HALO = 4


def split(v):
    high = v.astype(BF16).astype(F32)
    return jnp.concatenate([high, v - high], axis=1).astype(BF16)


def spreader(block, heads, rows):
    row = lax.broadcasted_iota(jnp.int32, (rows, LANES), 0)
    lane = lax.broadcasted_iota(jnp.int32, (rows, LANES), 1)
    row = jnp.where(row >= heads, row - heads, row)
    head = 2 * block + jnp.where(lane >= HEAD, 1, 0)
    return jnp.where(row == head, 1.0, 0.0).astype(BF16)


def dot(a, b):
    return jnp.dot(a, b, preferred_element_type=F32)


def silu(v):
    half = 0.5 * v
    return half + half * jnp.tanh(half)


def kernel(
    n, group, heads, kernel_taps,
    x_hbm, gate_hbm, proj_hbm, raw_hbm, cw_hbm, cb_hbm, sb_hbm, rate_hbm, skip_hbm,
    u, sumsq,
    xb, gb, xs, cf, cr, gf, gr, ef, er, gw, ext,
    proj_v, raw_v, cw_v, cb_v, sb_v, rate_v, skip_v,
    lhs, mf, mr, bt, cm,
    prev_v, next_v, tot_v, tots_v, totg_v, totr_v,
    send1, recv1, send2, recv2, send3, recv3,
    e_sem, x_sem, g_sem, s_sem, ready, h_send, h_recv,
    t1_send, t1_recv, t2_send, t2_recv, c1_send, c1_recv, c2_send, c2_recv, c3_send, c3_recv,
):
    rows = u.shape[1]
    blocks = u.shape[0]
    per = blocks // group
    groups = n // group
    states = bt.shape[1]
    me = lax.axis_index("seq")
    mem = lax.rem(me, group)
    grp = lax.div(me, group)
    base = me - mem

    def lanes(j):
        return pl.ds(pl.multiple_of(j * LANES, LANES), LANES)

    def pick(table, r):
        if isinstance(r, int):
            return table[r - 1]
        found = 0
        for k, value in enumerate(table):
            found = found + jnp.where(r == k + 1, value, 0)
        return found

    def offset(r, way):
        if group != 8:
            return lax.rem(mem + way * r + group, group)
        code = pick(NEAR, r)
        high, low = (divmod(code, 4)) if isinstance(code, int) else (lax.div(code, 4), lax.rem(code, 4))
        across = lax.rem(lax.div(mem, 4) + high, 2)
        return across * 4 + lax.rem(lax.rem(mem, 4) + way * low + 4, 4)

    def member(r):
        return offset(r, 1)

    def far(r):
        return lax.rem(grp + (pick(FAR, r) if groups == 8 else r), groups)

    def sweep(body, many):
        def turn(i, carry):
            for q in range(many):
                body(i * many + q)
            return carry

        lax.fori_loop(0, blocks // many, turn, 0)

    small = [
        (raw_hbm, raw_v), (sb_hbm, sb_v), (rate_hbm, rate_v), (proj_hbm, proj_v),
        (skip_hbm, skip_v), (cw_hbm, cw_v), (cb_hbm, cb_v),
    ]
    loads = [pltpu.make_async_copy(a, b, s_sem.at[i]) for i, (a, b) in enumerate(small)]
    bands = rows // BAND

    def x_copy(first, count, semaphore):
        band = pl.ds(first, count)
        return pltpu.make_async_copy(x_hbm.at[band], xb.at[band], semaphore)

    borders = [x_copy(0, EDGE, e_sem.at[0]), x_copy(rows - EDGE, EDGE, e_sem.at[1])]
    middle = x_copy(EDGE, rows - 2 * EDGE, x_sem)
    for copy in borders + loads + [middle]:
        copy.start()

    def g_copy(i):
        band = pl.ds(i * BAND, BAND)
        return pltpu.make_async_copy(gate_hbm.at[band], gb.at[band], g_sem)

    barrier = pltpu.get_barrier_semaphore()
    after = lax.rem(me + 1, n)
    before = lax.rem(me + n - 1, n)
    beside = (lax.rem(me + group, n), lax.rem(me + n - group, n))

    def signal(semaphore, peer):
        pl.semaphore_signal(semaphore, inc=1, device_id={"seq": peer}, device_id_type=MESH)

    for peer in (after, before) + beside:
        signal(barrier, peer)
    for r in range(1, group):
        signal(barrier, base + member(r))

    for i in range(bands):
        g_copy(i).start()

    pl.semaphore_wait(barrier, 4 + (group - 1))
    for copy in borders:
        copy.wait()
    halo = [
        pltpu.make_async_remote_copy(
            src_ref=xb.at[pl.ds(rows - HALO, HALO)], dst_ref=prev_v,
            send_sem=h_send.at[0], recv_sem=h_recv.at[0],
            device_id={"seq": after}, device_id_type=MESH,
        ),
        pltpu.make_async_remote_copy(
            src_ref=xb.at[pl.ds(0, HALO)], dst_ref=next_v,
            send_sem=h_send.at[1], recv_sem=h_recv.at[1],
            device_id={"seq": before}, device_id_type=MESH,
        ),
    ]
    for copy in halo:
        copy.start()
    rounds = groups // 2 - 1

    def relay(k):
        if 0 < k <= rounds:
            pl.semaphore_wait(ready.at[k - 1], 2)
        if k < rounds:
            for peer in beside:
                signal(ready.at[k], peer)

    relay(0)
    first_t = lax.broadcasted_iota(jnp.int32, (rows, rows), 0)
    second_t = lax.broadcasted_iota(jnp.int32, (rows, rows), 1)
    masks = (first_t >= second_t, first_t <= second_t)
    for copy in loads[:5]:
        copy.wait()

    lasts = (rows - 1, 0)
    raw = raw_v[...].astype(F32)
    params = jnp.concatenate(
        [
            jnp.concatenate([sb_v[...], rate_v[...], jnp.zeros((4, heads), F32)], axis=0),
            jnp.zeros((8, LANES - heads), F32),
        ],
        axis=1,
    ).T
    zeros = jnp.zeros((16 - 4, heads), F32)
    grow, decay, total, skips = [], [], [], []
    for d in range(2):
        v = raw[d * heads : (d + 1) * heads] + params[:heads, d : d + 1]
        step = jnp.maximum(v, 0.0) + jnp.log1p(jnp.exp(-jnp.abs(v)))
        cumul = jnp.dot(
            -params[:heads, 2 + d : 3 + d] * step,
            jnp.where(masks[1 - d], 1.0, 0.0),
            precision=lax.Precision.HIGHEST,
            preferred_element_type=F32,
        )
        grow.append((jnp.exp(-cumul) * step).T)
        decay.append(jnp.exp(cumul).T)
        total.append(decay[d][lasts[d] : lasts[d] + 1, :])
        skips.append(skip_v[d : d + 1, :])
        first = 2 * d * states
        write_t = proj_v[first : first + states, :]
        read = proj_v[first + states : first + 2 * states, :].astype(F32).T.astype(BF16)
        bt[d] = write_t
        cm[d] = read
        scores = jnp.where(masks[d], dot(read, write_t), 0.0).astype(BF16)
        (mf, mr)[d][...] = scores
    lhs[...] = split(jnp.concatenate(decay + grow + total + skips + [zeros], axis=0))
    tot_v[...] = jnp.concatenate(
        [
            jnp.concatenate(total, axis=0),
            jnp.zeros((2, LANES - heads), F32),
        ],
        axis=1,
    )

    def near_copy(src, dst, ss, rs, r):
        return pltpu.make_async_remote_copy(
            src_ref=src, dst_ref=dst, send_sem=ss, recv_sem=rs,
            device_id={"seq": base + member(r)}, device_id_type=MESH,
        )

    def far_copy(src, dst, ss, rs, r):
        return pltpu.make_async_remote_copy(
            src_ref=src, dst_ref=dst, send_sem=ss, recv_sem=rs,
            device_id={"seq": far(r) * group + mem}, device_id_type=MESH,
        )

    def t1(r):
        return near_copy(tot_v, tots_v.at[mem], t1_send, t1_recv, r)

    def t2(r):
        return far_copy(totg_v, totr_v.at[grp], t2_send, t2_recv, r)

    def c1(r):
        return near_copy(send1.at[member(r)], recv1.at[mem], c1_send, c1_recv, r)

    def c2(r, b):
        ahead = jnp.where(far(r) > grp, 0, 1)
        return far_copy(
            send2.at[ahead, b], recv2.at[b, grp], c2_send.at[b], c2_recv.at[b], r
        )

    def c3(r, b):
        return near_copy(
            send3.at[b, member(r)], recv3.at[b, mem], c3_send.at[b], c3_recv.at[b], r
        )

    near_all, far_all = pl.ds(0, group - 1), pl.ds(0, groups - 1)
    t1_all = near_copy(tots_v.at[near_all], tots_v.at[near_all], t1_send, t1_recv, 1)
    t2_all = far_copy(totr_v.at[far_all], totr_v.at[far_all], t2_send, t2_recv, 1)
    c1_all = near_copy(send1.at[near_all], recv1.at[near_all], c1_send, c1_recv, 1)

    def c2_all(b):
        whole = recv2.at[b, far_all]
        return far_copy(whole, whole, c2_send.at[b], c2_recv.at[b], 1)

    def c3_all(b):
        return near_copy(
            send3.at[b, near_all], recv3.at[b, near_all], c3_send.at[b], c3_recv.at[b], 1
        )


    def loop(first, last, action):
        def body(r, carry):
            action(r)
            return carry

        lax.fori_loop(first, last, body, 0)

    for r in range(1, group):
        t1(r).start()
    tots_v[mem] = tot_v[...]

    def growth(j):
        wide = dot(lhs[pl.ds(2 * rows, 2 * rows + 16), :], spreader(j, heads, 2 * heads))
        gw[0, j] = wide[:rows]
        gw[1, j] = wide[rows : 2 * rows]
        ext[j] = wide[2 * rows : 2 * rows + 8]

    sweep(growth, 12)
    relay(1)
    for copy in loads[5:]:
        copy.wait()
    middle.wait()
    for copy in halo:
        copy.wait()

    has_before = jnp.where(me > 0, 1.0, 0.0)
    has_after = jnp.where(me < n - 1, 1.0, 0.0)

    def conv(owner):
        for b in range(per):
            j = owner * per + b
            xs[j, pl.ds(8 - HALO, HALO), :] = prev_v[:, lanes(j)].astype(F32) * has_before
            xs[j, pl.ds(8 + rows, HALO), :] = next_v[:, lanes(j)].astype(F32) * has_after
            xs[j, pl.ds(8, rows), :] = xb[:, lanes(j)].astype(F32)
        for b in range(per):
            j = owner * per + b
            for d in range(2):
                acc = 0.5 * cb_v[d : d + 1, lanes(j)]
                for k in range(kernel_taps):
                    shift = -k if d == 0 else k
                    tap = 0.5 * cw_v[d, k : k + 1, lanes(j)]
                    acc = acc + tap * xs[j, pl.ds(8 + shift, rows), :]
                conved = (acc + acc * jnp.tanh(acc)).astype(BF16)
                (cf, cr)[d][j] = conved
                (gf, gr)[d][j] = (gw[d, j] * conved.astype(F32)).astype(BF16)

    def finish(owner, buffer):
        results = []
        for b in range(per):
            j = owner * per + b
            for d in range(2):
                end = dot(bt[d], (gf, gr)[d][j]) * ext[j, pl.ds(d, 1), :]
                results.append((b, d, end.astype(BF16)))
        for b, d, end in results:
            buffer[owner, b, pl.ds(d * states, states), :] = end

    conv(member(1))

    def ends(r):
        finish(member(r), send1)
        conv(member(r + 1))
        c1(r).start()

    loop(1, group - 1, ends)
    finish(member(group - 1), send1)
    c1(group - 1).start()
    conv(mem)
    finish(mem, recv1)
    relay(2)

    t1_all.wait()
    product = tots_v[0]
    for m in range(1, group):
        product = product * tots_v[m]
    totg_v[...] = product
    totr_v[grp] = product
    pltpu.make_async_copy(gate_hbm, gb, g_sem).wait()

    def inner(j):
        wide = dot(lhs[pl.ds(0, 2 * rows), :], spreader(j, heads, 2 * heads))
        gate = silu(gb[:, lanes(j)].astype(F32))
        far_f, far_r = wide[:rows] * gate, wide[rows:] * gate
        ef[j] = far_f
        er[j] = far_r
        direct = (
            ext[j, pl.ds(2, 1), :] * cf[j].astype(F32) + ext[j, pl.ds(3, 1), :] * cr[j].astype(F32)
        )
        u[j] = direct * gate + far_f * dot(mf[...], gf[j]) + far_r * dot(mr[...], gr[j])

    sweep(inner, 4)
    relay(3)
    for r in range(1, groups):
        t2(r).start()

    c1_all.wait_recv()

    def spread(values, b):
        flat = values[...].reshape(-1, LANES)
        high = flat.astype(BF16)
        low = (flat - high.astype(F32)).astype(BF16)
        ones = spreader(mem * per + b, LANES, LANES)
        return dot(high, ones) + dot(low, ones)

    near_t = [spread(tots_v, b) for b in range(per)]

    def part(ref, m, b, d):
        return ref[m, b, pl.ds(d * states, states), :].astype(F32)

    for b in range(per):
        run_f = jnp.zeros((states, LANES), F32)
        run_r = jnp.zeros((states, LANES), F32)
        for m in range(group):
            run_f = run_f * near_t[b][2 * m : 2 * m + 1] + part(recv1, m, b, 0)
            k = group - 1 - m
            run_r = run_r * near_t[b][2 * k + 1 : 2 * k + 2] + part(recv1, k, b, 1)
        send2[0, b] = run_f.astype(BF16)
        send2[1, b] = run_r.astype(BF16)
        for r in range(1, groups):
            c2(r, b).start()
    t2_all.wait()
    far_t = [spread(totr_v, b) for b in range(per)]
    for b in range(per):
        recv2[b, grp] = send2[0, b]

    for b in range(per):
        c2_all(b).wait_recv()
        run_f = jnp.zeros((states, LANES), F32)
        run_r = jnp.zeros((states, LANES), F32)
        for g in range(groups):
            new = run_f * far_t[b][2 * g : 2 * g + 1] + recv2[b, g].astype(F32)
            run_f = jnp.where(g < grp, new, run_f)
            k = groups - 1 - g
            new = run_r * far_t[b][2 * k + 1 : 2 * k + 2] + recv2[b, k].astype(F32)
            run_r = jnp.where(k > grp, new, run_r)
        for m in range(group):
            send3[b, m, pl.ds(0, states), :] = run_f.astype(BF16)
            run_f = run_f * near_t[b][2 * m : 2 * m + 1] + part(recv1, m, b, 0)
            k = group - 1 - m
            send3[b, k, pl.ds(states, states), :] = run_r.astype(BF16)
            run_r = run_r * near_t[b][2 * k + 1 : 2 * k + 2] + part(recv1, k, b, 1)
        for r in range(1, group):
            c3(r, b).start()
        recv3[b, mem] = send3[b, mem]

    sumsq[...] = jnp.zeros_like(sumsq)
    many = min(8, group)
    for b in range(per):
        c3_all(b).wait_recv()

        def outer(i, carry):
            squares = jnp.zeros((rows, LANES), F32)
            for q in range(many):
                owner = i * many + q
                j = owner * per + b
                gated = (
                    u[j]
                    + ef[j] * dot(cm[0], recv3[b, owner, pl.ds(0, states), :])
                    + er[j] * dot(cm[1], recv3[b, owner, pl.ds(states, states), :])
                )
                u[j] = gated
                squares = squares + gated * gated
            sumsq[...] += squares
            return carry

        lax.fori_loop(0, group // many, outer, 0)

    c1_all.wait_send()
    for b in range(per):
        c2_all(b).wait_send()
        c3_all(b).wait_send()


def finale(u, sumsq, gain, out_hbm, ob, o_sem):
    blocks, rows, _ = u.shape
    mean = jnp.sum(sumsq[...], axis=1, keepdims=True) * (1.0 / (blocks * LANES))
    scale = lax.rsqrt(mean + 1e-05)
    for i in range(rows // 16):
        part = slice(i * 16, (i + 1) * 16)
        for j in range(blocks):
            lanes = slice(j * LANES, (j + 1) * LANES)
            ob[part, lanes] = (u[j, part] * scale[part] * gain[:, lanes]).astype(BF16)
        band = pl.ds(i * 16, 16)
        pltpu.make_async_copy(ob.at[band], out_hbm.at[band], o_sem).start()
    pltpu.make_async_copy(ob, out_hbm, o_sem).wait()


def solution(mesh, group=GROUP):
    n = mesh.shape["seq"]

    def local(inner, gate, proj, raw, conv_weight, conv_bias, step_bias, rate, skip, gain):
        rows, width = inner.shape
        heads = width // HEAD
        blocks = width // LANES
        per = blocks // group
        groups = n // group
        states = proj.shape[1] // 4
        taps = conv_weight.shape[1]
        dma = pltpu.SemaphoreType.DMA
        vm = pltpu.VMEM
        wide16 = vm((blocks, rows, LANES), BF16)
        wide32 = vm((blocks, rows, LANES), F32)
        scratch = [
            vm((rows, width), BF16),
            vm((rows, width), BF16),
            vm((blocks, rows + 16, LANES), F32),
            wide16,
            wide16,
            wide16,
            wide16,
            wide32,
            wide32,
            vm((2, blocks, rows, LANES), F32),
            vm((blocks, 8, LANES), F32),
            vm(proj.shape[::-1], BF16),
            vm(raw.shape[::-1], BF16),
            vm(conv_weight.shape, F32),
            vm(conv_bias.shape, F32),
            vm(step_bias.shape, F32),
            vm(rate.shape, F32),
            vm(skip.shape, F32),
            vm((4 * rows + 16, 2 * heads), BF16),
            vm((rows, rows), BF16),
            vm((rows, rows), BF16),
            vm((2, states, rows), BF16),
            vm((2, rows, states), BF16),
            vm((HALO, width), BF16),
            vm((HALO, width), BF16),
            vm((2, LANES), F32),
            vm((group, 2, LANES), F32),
            vm((2, LANES), F32),
            vm((groups, 2, LANES), F32),
            vm((group, per, 2 * states, LANES), BF16),
            vm((group, per, 2 * states, LANES), BF16),
            vm((2, per, states, LANES), BF16),
            vm((per, groups, states, LANES), BF16),
            vm((per, group, 2 * states, LANES), BF16),
            vm((per, group, 2 * states, LANES), BF16),
            dma((2,)),
            dma,
            dma,
            dma((7,)),
            pltpu.SemaphoreType.REGULAR((max(1, groups // 2 - 1),)),
            dma((2,)),
            dma((2,)),
        ]
        scratch += [dma] * 6 + [dma((per,))] * 4
        vmem = pl.BlockSpec(memory_space=pltpu.VMEM)
        hbm = pl.BlockSpec(memory_space=pl.ANY)
        gated, sumsq = pl.pallas_call(
            functools.partial(kernel, n, group, heads, taps),
            out_shape=(
                jax.ShapeDtypeStruct((blocks, rows, LANES), F32),
                jax.ShapeDtypeStruct((rows, LANES), F32),
            ),
            in_specs=[hbm] * 9,
            out_specs=(vmem, vmem),
            scratch_shapes=scratch,
            compiler_params=pltpu.CompilerParams(
                collective_id=0, has_side_effects=True, vmem_limit_bytes=36 * 2**20
            ),
            name="mixer",
        )(
            *(
                pltpu.with_memory_space_constraint(array, pltpu.HBM)
                for array in (
                    inner, gate, proj.T, raw.T, conv_weight, conv_bias, step_bias, rate, skip
                )
            )
        )
        return pl.pallas_call(
            finale,
            out_shape=jax.ShapeDtypeStruct((rows, width), BF16),
            in_specs=[vmem, vmem, vmem],
            out_specs=hbm,
            scratch_shapes=[vm((rows, width), BF16), dma],
            compiler_params=pltpu.CompilerParams(vmem_limit_bytes=16 * 2**20),
            name="finale",
        )(gated, sumsq, gain.reshape(1, width))

    spec = P(("img", "seq"), None)
    return jax.shard_map(
        local,
        mesh=mesh,
        in_specs=(spec, spec, spec, spec, P(), P(), P(), P(), P(), P()),
        out_specs=spec,
        check_vma=False,
    )
```
